256 devices in a mesh: pa: 16 (over x_hi, z), gz: 16 (over x_lo, y, core).
Axes of the slice: x: 4 (x_hi: 2, x_lo: 2; x = x_hi * 2 + x_lo), y: 4, z: 8, core: 2. Of those that a mesh axis runs over, the one named last changes fastest.
Arguments:
- source: float32 [128, 768, 768], P('gz', 'pa'), may hold values from -24 to 24
- cell_width: float32 [128], P('gz'), may hold values from 0.5 to 2
Outputs:
- potential: float32 [128, 768, 768], P('gz', 'pa')
The draws below stay inside these ranges and needn't reach their ends.
All inputs are finite; a program needn't handle non-finite values.
Results may differ from the reference program's by a relative error of at most 0.00085.
Values sent between devices are 32-bit elements; how exact they have to be, the bound alone decides.
A program may use at most 64 MiB of HBM per device.

```python
import math
import jax
import jax.numpy as jnp
from jax import lax

NX = 768
NY = 768
NZ = 128


def laplace_field(field):
    mirrored = jnp.concatenate([field[:, :, :1], field, field[:, :, -1:]], 2)
    across = 2.0 * field - mirrored[:, :, :-2] - mirrored[:, :, 2:]
    padded_rows = jnp.pad(field, ((0, 0), (1, 1), (0, 0)))
    columns = 2.0 * field - padded_rows[:, :-2, :] - padded_rows[:, 2:, :]
    padded_depth = jnp.pad(field, ((1, 1), (0, 0), (0, 0)))
    along_depth = 2.0 * field - padded_depth[:-2] - padded_depth[2:]
    return across + columns + along_depth


def draw_source(key, part):
    rough = jnp.clip(jax.random.normal(key, (NZ, NY, NX), jnp.float32), -4.0, 4.0)
    return 0.5 * laplace_field(rough)


def shard_levels(stream_key, shape, shards, smallest, top_value):
    gain, own = 1.0, jax.random.fold_in(stream_key, 6)
    for dim, shards_of in shards:
        heights = jnp.exp(jax.random.uniform(jax.random.fold_in(own, dim), (shards_of,), jnp.float32, smallest / len(shards), top_value / len(shards)))
        gain = gain * jnp.repeat(heights, shape[dim] // shards_of).reshape([-1 if axis == dim else 1 for axis in range(len(shape))])
    return gain


def setup_inputs(seed: int = 0) -> dict:
    splits = jax.random.split(jax.random.key(seed), 3)
    return {
        "source": draw_source(jax.random.fold_in(splits[2], 71), 0),
        "cell_width": jnp.clip(jnp.exp(math.log(2.0) - 1.3862944 * jax.random.uniform(splits[1], (NZ,), jnp.float32) ** shard_levels(splits[1], (NZ,), ((0, 16),), -0.2, 0.2)), 0.5, 2.0),
    }


HIGHEST = lax.Precision.HIGHEST

def cosine_table(width):
    counter = jnp.arange(width, dtype=jnp.int32)
    phases = counter[:, None] * (2 * counter[None, :] + 1) % (4 * width)
    angles = phases.astype(jnp.float32) * (math.pi / (2 * width))
    weights = jnp.where(counter == 0, math.sqrt(1.0 / width), math.sqrt(2.0 / width)).astype(jnp.float32)
    return weights[:, None] * jnp.cos(angles)

def sine_table(width):
    counter = jnp.arange(1, width + 1, dtype=jnp.int32)
    phases = counter[:, None] * counter[None, :] % (2 * (width + 1))
    angles = phases.astype(jnp.float32) * (math.pi / (width + 1))
    return math.sqrt(2.0 / (width + 1)) * jnp.sin(angles)

def eigen_first(offset, count, width):
    wavenumber = (offset + jnp.arange(count, dtype=jnp.int32)).astype(jnp.float32)
    return 4.0 * jnp.square(jnp.sin(wavenumber * (math.pi / (2 * width))))

def eigen_second(width):
    wavenumber = jnp.arange(1, width + 1, dtype=jnp.int32).astype(jnp.float32)
    return 4.0 * jnp.square(jnp.sin(wavenumber * (math.pi / (2 * (width + 1)))))

def reference(source, cell_width):
    cos_table = cosine_table(NX)
    sin_table = sine_table(NY)
    padded = jnp.pad(cell_width, 1)
    upper_coef = 2.0 / (padded[1:-1] + padded[2:])
    lower_coef = 2.0 / (padded[:-2] + padded[1:-1])
    along_x = jnp.einsum('zyi,ki->zky', source, cos_table, precision=HIGHEST)
    spectral = jnp.einsum('zkj,lj->zkl', along_x, sin_table, precision=HIGHEST)
    eigen_sum = eigen_first(0, NX, NX)[:, None] + eigen_second(NY)[None, :]

    def eliminate(previous, entries):
        below_coef, above_coef, width_cell, forcing = entries
        diagonal = below_coef + above_coef + width_cell * eigen_sum
        divisor = diagonal + below_coef * previous[0]
        ratio_now = -above_coef / divisor
        value_now = (width_cell * forcing + below_coef * previous[1]) / divisor
        return ((ratio_now, value_now), (ratio_now, value_now))
    zero_plane = jnp.zeros((NX, NY), jnp.float32)
    _, (ratios, values) = lax.scan(eliminate, (zero_plane, zero_plane), (lower_coef, upper_coef, cell_width, spectral))

    def substitute(following, entries):
        current = entries[1] - entries[0] * following
        return (current, current)
    _, solved = lax.scan(substitute, zero_plane, (ratios, values), reverse=True)
    along_y = jnp.einsum('zkl,lj->zkj', solved, sin_table, precision=HIGHEST)
    return jnp.einsum('zky,ki->zyi', along_y, cos_table, precision=HIGHEST)
```

```python
import functools

import jax
import jax.numpy as jnp
import numpy as np
from jax import lax
from jax.experimental import pallas as pl
from jax.experimental.pallas import tpu as pltpu
from jax.sharding import PartitionSpec as P

F32 = jnp.float32
BF16 = jnp.bfloat16
N = 768
NB = 16
ZL = 8
YL = 48
LANES = 128
CH = N // LANES
SOLVERS = tuple(g for g in range(NB) if g not in (0, 4, 10, 14))
NS = len(SOLVERS)
HALF = N // 2


def split64(x):
    hi = x.astype(np.float32).astype(jnp.bfloat16)
    lo = (x - hi.astype(np.float64)).astype(np.float32).astype(jnp.bfloat16)
    return np.stack([hi, lo])


@functools.cache
def tables():
    n = np.arange(N)
    phases = n[:, None] * (2 * n[None, :] + 1) % (4 * N)
    weights = np.where(n == 0, np.sqrt(1.0 / N), np.sqrt(2.0 / N))
    cos_t = weights[:, None] * np.cos(phases * (np.pi / (2 * N)))

    def sine(width, rows, cols):
        p = rows[:, None] * cols[None, :] % (2 * (width + 1))
        return np.sqrt(2.0 / (width + 1)) * np.sin(p * (np.pi / (width + 1)))

    m = n + 1
    sin_t = sine(N, m, m)
    ml = np.arange(1, YL + 1)
    s48 = sine(YL, ml, ml)
    hi, lo = split64(s48)
    s48st = np.concatenate([hi, hi, lo], axis=1)
    mc = np.zeros((ZL * YL, LANES))
    mc[:YL, :YL] = s48
    mc[(ZL - 1) * YL :, YL : 2 * YL] = s48
    for z in range(ZL):
        mc[z * YL : (z + 1) * YL, 2 * YL + 2 * z] = s48[:, 0]
        mc[z * YL : (z + 1) * YL, 2 * YL + 2 * z + 1] = s48[:, YL - 1]
    own = np.zeros((NB, ZL, 2, N))
    beside = np.zeros((NB, ZL, 2, N))
    for p in range(NB):
        for e in range(2):
            row = YL * p + (YL - 1) * e
            own[p, :, e] = sin_t[row]
            near = row + (1 if e else -1)
            if 0 <= near < N:
                beside[p, :, e] = sin_t[near]
    own = own.reshape(2 * ZL * NB, N)
    beside = beside.reshape(2 * ZL * NB, N)
    lam_k = 4 * np.sin(n * np.pi / (2 * N)) ** 2
    lam_l = 4 * np.sin(m * np.pi / (2 * (N + 1))) ** 2
    lam_s = 4 * np.sin(ml * np.pi / (2 * (YL + 1))) ** 2
    rows = np.zeros((8, N), np.float32)
    rows[0] = lam_k
    rows[1] = lam_l
    return dict(
        cos=split64(cos_t),
        sin=split64(sin_t),
        s48=s48st,
        mct=split64(mc.T.copy()),
        mc=split64(mc),
        win=split64(own),
        wout=split64(beside.T.copy()),
        rows=rows,
        lam_s=np.broadcast_to(lam_s[:, None], (YL, LANES)).astype(np.float32),
        lam_k=np.broadcast_to(lam_k[:, None], (N, LANES)).astype(np.float32),
    )


TABLES = ("cos", "sin", "s48", "mct", "mc", "win", "wout", "rows", "lam_s", "lam_k")


def cut(x):
    hi = x.astype(BF16)
    return hi, (x - hi.astype(F32)).astype(BF16)


def dot(a, b):
    return jnp.dot(a, b, preferred_element_type=F32)


def dot_nt(a, b):
    return lax.dot_general(a, b, (((1,), (1,)), ((), ())), preferred_element_type=F32)


def by_table(x, hi, lo, f=dot):
    a, b = cut(x)
    return f(a, hi) + f(b, hi) + f(a, lo)


def table_by(hi, lo, x):
    a, b = cut(x)
    return dot(hi, a) + dot(hi, b) + dot(lo, a)


def recip(x):
    return 1.0 / x


def lane_iota(rows):
    return lax.broadcasted_iota(jnp.int32, (rows, LANES), 1)


def remote(src, dst, send, recv, where):
    return pltpu.make_async_remote_copy(
        src_ref=src,
        dst_ref=dst,
        send_sem=send,
        recv_sem=recv,
        device_id=where,
        device_id_type=pl.DeviceIdType.MESH,
    )


def rolled(x, shift):
    shift %= LANES
    return x if shift == 0 else pltpu.roll(x, shift, axis=1)


def kernel(
    src, cw, cos_r, sin_r, s48, mct, mc, win, wout, lam_rows, lam_s, lam_k, out,
    s_hi, s_lo, fh, work, eloc, pbuf, precv, wmine, widths, alpha, beta, planes, rhy, eg,
    qbuf, qrecv, rbuf, rrecv, c00, c70, c70c, ci, cia, cc, hh, bbuf, brecv, scale,
    psend_s, precv_s, wsend_s, wrecv_s, qsend_s, qrecv_s, rsend_s, rrecv_s, bsend_s, brecv_s,
):
    pa = lax.axis_index("pa")
    gz = lax.axis_index("gz")

    def peer(me, d):
        return lax.rem(me + d, NB)

    barrier = pltpu.get_barrier_semaphore()
    for d in range(1, NB):
        pl.semaphore_signal(barrier, inc=1, device_id={"pa": peer(pa, d)}, device_id_type=pl.DeviceIdType.MESH)
        pl.semaphore_signal(barrier, inc=1, device_id={"gz": peer(gz, d)}, device_id_type=pl.DeviceIdType.MESH)

    for z in range(ZL):
        wmine[z : z + 1, :] = jnp.full((1, LANES), cw[z], F32)
    x = src[...]
    a, b = cut(x)
    s_hi[...] = a
    s_lo[...] = b

    def forward(c):
        cols = slice(c * 256, (c + 1) * 256)
        hi = cos_r[0, cols, :]
        lo = cos_r[1, cols, :]
        f = dot_nt(s_hi[...], hi) + dot_nt(s_lo[...], hi) + dot_nt(s_hi[...], lo)
        for z in range(ZL):
            a, b = cut(f[z * YL : (z + 1) * YL])
            fh[z, :, cols] = dot(s48[...], jnp.concatenate([a, b, a], axis=0))

    forward(0)
    pl.semaphore_wait(barrier, 2 * (NB - 1))
    wcopies = [
        remote(wmine, widths.at[gz], wsend_s.at[d], wrecv_s.at[gz], {"gz": peer(gz, d)})
        for d in range(1, NB)
    ]
    for copy in wcopies:
        copy.start()
    widths[gz] = wmine[...]
    forward(1)
    forward(2)
    for copy in wcopies:
        copy.wait_send()
    for d in range(1, NB):
        g = peer(gz, d)
        remote(wmine, widths.at[g], wsend_s.at[d], wrecv_s.at[g], {"gz": g}).wait_recv()

    w = widths[...].reshape(NB * ZL, LANES)
    at = lax.broadcasted_iota(jnp.int32, (NB * ZL, LANES), 0)
    before = jnp.where(at == 0, 0.0, pltpu.roll(w, 1, axis=0))
    after = jnp.where(at == NB * ZL - 1, 0.0, pltpu.roll(w, NB * ZL - 1, axis=0))
    alpha[...] = 2.0 / ((before + w) * w)
    beta[...] = 2.0 / ((w + after) * w)
    mine = pl.ds(pl.multiple_of(gz * ZL, ZL), ZL)
    al_b = alpha[mine, :]
    be_b = beta[mine, :]

    def a_of(z, like):
        return jnp.broadcast_to(al_b[z : z + 1, :], like)

    def b_of(z, like):
        return jnp.broadcast_to(be_b[z : z + 1, :], like)

    tile = (YL, LANES)

    def factor(e_ref, cols, lam):
        e = None
        for z in range(ZL):
            d = a_of(z, tile) + b_of(z, tile) + lam
            if z:
                d = d - a_of(z, tile) * b_of(z - 1, tile) * e
            e = recip(d)
            e_ref[z, :, cols] = e

    def solve(rhs_of, e_ref, cols, x_ref):
        y = None
        for z in range(ZL):
            r = rhs_of(z)
            if z:
                r = r + a_of(z, tile) * y
            y = e_ref[z, :, cols] * r
            x_ref[z, :, cols] = y
        first = y
        last = y
        for z in range(ZL - 2, -1, -1):
            first = x_ref[z, :, cols] + e_ref[z, :, cols] * b_of(z, tile) * first
            x_ref[z, :, cols] = first
        return first, last

    def block(c):
        cols = pl.ds(pl.multiple_of(c * LANES, LANES), LANES)
        lam = lam_s[...] + lam_rows[0:1, cols]
        factor(eloc, cols, lam)
        solve(lambda z: fh[z, :, cols], eloc, cols, work)
        v = work[:, :, cols].reshape(ZL * YL, LANES)
        p = table_by(mct[0], mct[1], v)
        pbuf[cols, :] = jnp.transpose(p)

    pl.loop(0, CH)(block)

    def mine48(ref, q):
        return ref.at[pl.ds(pl.multiple_of(q * YL, YL), YL), :]

    pcopies = [
        remote(mine48(pbuf, peer(pa, d)), precv.at[pa], psend_s.at[d], precv_s.at[pa], {"pa": peer(pa, d)})
        for d in range(1, NB)
    ]
    for copy in pcopies:
        copy.start()
    precv[pa] = pbuf[pl.ds(pl.multiple_of(pa * YL, YL), YL), :]

    lk = lam_k[pl.ds(pl.multiple_of(pa * YL, YL), YL), :]

    def global_factor(c):
        cols = pl.ds(pl.multiple_of(c * LANES, LANES), LANES)
        factor(eg, cols, lk + lam_rows[1:2, cols])

    pl.loop(0, CH)(global_factor)

    idle_before = sum(((gz > g).astype(jnp.int32) for g in (0, 4, 10, 14)), jnp.int32(0))
    me_s = gz - idle_before
    is_solver = (gz != 0) & (gz != 4) & (gz != 10) & (gz != 14)
    krow = lam_k[pl.ds(pl.multiple_of(pa * YL + 8 * lax.div(me_s, 2), 8), 8), :]
    half = lax.rem(me_s, 2)

    def row_of(ref, i):
        v = ref[pl.ds(i, 1), :]
        return jnp.broadcast_to(jnp.concatenate([v, v, v], axis=1), (8, HALF))

    @pl.when(is_solver)
    def _():
        lam = jnp.concatenate([krow, krow, krow], axis=1) + lam_rows[
            1:2, pl.ds(pl.multiple_of(half * HALF, HALF), HALF)
        ]

        def coefficients(b, carry):
            al = [row_of(alpha, b * ZL + z) for z in range(ZL)]
            be = [row_of(beta, b * ZL + z) for z in range(ZL)]
            e = recip(al[0] + be[0] + lam)
            prod_e = e
            prod_a = al[0]
            prod_b = be[0]
            for z in range(1, ZL):
                e = recip(al[z] + be[z] + lam - al[z] * be[z - 1] * e)
                prod_e = prod_e * e * al[z]
                prod_b = prod_b * be[z] / al[z]
            a70 = prod_e * prod_a
            a07 = prod_e * prod_b
            a77 = e * be[ZL - 1]
            g = recip(al[ZL - 1] + be[ZL - 1] + lam)
            for z in range(ZL - 2, -1, -1):
                g = recip(al[z] + be[z] + lam - be[z] * al[z + 1] * g)
            a00 = g * al[0]
            c00[b] = a00
            c70[b] = a70
            cia[b] = a07
            cc[b] = a77
            return carry

        lax.fori_loop(0, NB, coefficients, 0)
        c = jnp.zeros((8, HALF), F32)
        for b in range(NB):
            inv = recip(1.0 - c00[b] * c)
            ia = inv * cia[b]
            bc = c70[b] * c
            ci[b] = inv
            cia[b] = ia
            c70c[b] = bc
            c = cc[b] + bc * ia
            cc[b] = c

    for copy in pcopies:
        copy.wait_send()
    for d in range(1, NB):
        p = peer(pa, d)
        remote(mine48(pbuf, p), precv.at[p], psend_s.at[d], precv_s.at[p], {"pa": p}).wait_recv()

    lanes = lane_iota(YL)
    zero = jnp.zeros(tile, F32)

    def gathered(base, t):
        value = zero
        for p in range(NB):
            start = YL * p - LANES * t
            if start + YL <= 0 or start >= LANES:
                continue
            piece = rolled(precv[p], start - base)
            value = jnp.where((lanes >= start) & (lanes < start + YL), piece, value)
        return value

    for t in range(CH):
        planes[0:YL, t * LANES : (t + 1) * LANES] = gathered(0, t)
        planes[YL : 2 * YL, t * LANES : (t + 1) * LANES] = gathered(YL, t)

    def beside(t):
        value = zero
        odd = lax.rem(lanes, 2) == 1
        for p in range(8 * t, 8 * t + 8):
            at_p = (lanes >= 16 * (p - 8 * t)) & (lanes < 16 * (p - 8 * t) + 16)
            start = 16 * (p - 8 * t) - 2 * YL
            if p > 0:
                value = jnp.where(at_p & ~odd, rolled(precv[p - 1], start - 1), value)
            if p < NB - 1:
                value = jnp.where(at_p & odd, rolled(precv[p + 1], start + 1), value)
        return value

    near = [beside(t) for t in range(2)]
    at_z = [lax.div(lax.rem(lanes, 16), 2) == z for z in range(ZL)]
    for z in range(ZL):
        a, b = cut(jnp.concatenate([jnp.where(at_z[z], v, 0.0) for v in near], axis=1))
        s_hi[z * YL : (z + 1) * YL, 0:256] = a
        s_lo[z * YL : (z + 1) * YL, 0:256] = b

    for n in range(3):
        cols = slice(n * 256, (n + 1) * 256)
        r = dot(s_hi[:, 0:256], win[0, :, cols])
        r = r + dot(s_lo[:, 0:256], win[0, :, cols]) + dot(s_hi[:, 0:256], win[1, :, cols])
        rhy[:, :, cols] = r.reshape(ZL, YL, 256)
    ph, plo = cut(planes[...])
    for n in range(3):
        cols = slice(n * 256, (n + 1) * 256)
        r = dot(ph, sin_r[0, :, cols]) + dot(plo, sin_r[0, :, cols]) + dot(ph, sin_r[1, :, cols])
        planes[:, cols] = r
    for c in range(CH):
        cols = slice(c * LANES, (c + 1) * LANES)
        first, last = solve(lambda z: rhy[z, :, cols], eg, cols, work)
        q0 = planes[0:YL, cols] + first
        q7 = planes[YL : 2 * YL, cols] + last
        there = slice((c % 3) * LANES, (c % 3 + 1) * LANES)
        for rt in range(YL // 8):
            qbuf[2 * rt + c // 3, 0, :, there] = q0[8 * rt : 8 * rt + 8]
            qbuf[2 * rt + c // 3, 1, :, there] = q7[8 * rt : 8 * rt + 8]

    for s, g in enumerate(SOLVERS):

        @pl.when(gz != g)
        def _():
            remote(qbuf.at[s], qrecv.at[gz], qsend_s.at[s], qrecv_s.at[gz], {"gz": g}).start()

        @pl.when(gz == g)
        def _():
            qrecv[gz] = qbuf[s]

    @pl.when(is_solver)
    def _():
        for d in range(1, NB):
            g = peer(gz, d)
            remote(qbuf.at[0], qrecv.at[g], qsend_s.at[0], qrecv_s.at[g], {"gz": g}).wait_recv()
        s = jnp.zeros((8, HALF), F32)
        for b in range(NB):
            rbuf[b, 0] = s
            h = ci[b] * (qrecv[b, 0] + c00[b] * s)
            hh[b] = h
            s = qrecv[b, 1] + c70[b] * s + c70c[b] * h
        value = jnp.zeros((8, HALF), F32)
        for b in range(NB - 1, -1, -1):
            rbuf[b, 1] = value
            if b:
                upper = hh[b] + cia[b] * value
                rbuf[b, 0] = rbuf[b, 0] + cc[b - 1] * upper
                value = upper
        for d in range(1, NB):
            g = peer(gz, d)
            remote(rbuf.at[g], rrecv.at[me_s], rsend_s.at[d], rrecv_s.at[me_s], {"gz": g}).start()
        rrecv[me_s] = rbuf[gz]

    for s, g in enumerate(SOLVERS):

        @pl.when(gz != g)
        def _():
            remote(qbuf.at[s], qrecv.at[gz], qsend_s.at[s], qrecv_s.at[gz], {"gz": g}).wait_send()
            remote(rbuf.at[0], rrecv.at[s], rsend_s.at[0], rrecv_s.at[s], {"gz": g}).wait_recv()

    for c in range(CH):
        cols = slice(c * LANES, (c + 1) * LANES)
        there = slice((c % 3) * LANES, (c % 3 + 1) * LANES)
        low = jnp.concatenate([rrecv[2 * rt + c // 3, 0, :, there] for rt in range(YL // 8)], axis=0)
        high = jnp.concatenate([rrecv[2 * rt + c // 3, 1, :, there] for rt in range(YL // 8)], axis=0)
        planes[0:YL, cols] = low
        planes[YL : 2 * YL, cols] = high

        def full(z):
            r = rhy[z, :, cols]
            if z == 0:
                r = r + a_of(0, tile) * low
            if z == ZL - 1:
                r = r + b_of(ZL - 1, tile) * high
            return r

        solve(full, eg, cols, work)
    a, b = cut(work[...].reshape(ZL * YL, N))
    r = dot(a, wout[0]) + dot(b, wout[0]) + dot(a, wout[1])
    edge = []
    for t in range(2):
        value = near[t]
        for z in range(ZL):
            value = value + jnp.where(at_z[z], r[z * YL : (z + 1) * YL, t * LANES : (t + 1) * LANES], 0.0)
        edge.append(value)
    ph, plo = cut(planes[...])
    for n in range(3):
        cols = slice(n * 256, (n + 1) * 256)
        r = dot(ph, sin_r[0, :, cols]) + dot(plo, sin_r[0, :, cols]) + dot(ph, sin_r[1, :, cols])
        planes[:, cols] = r
    for p in range(NB):
        value = zero
        for half_p in range(2):
            t0 = YL * p // LANES
            for t in range(t0, (YL * p + YL - 1) // LANES + 1):
                shift = LANES * t - YL * p + YL * half_p
                first = max(LANES * t, YL * p) - YL * p + YL * half_p
                stop = min(LANES * (t + 1), YL * p + YL) - YL * p + YL * half_p
                piece = rolled(planes[half_p * YL : (half_p + 1) * YL, t * LANES : (t + 1) * LANES], shift)
                value = jnp.where((lanes >= first) & (lanes < stop), piece, value)
        piece = rolled(edge[p // 8], 2 * YL - 16 * (p % 8))
        value = jnp.where((lanes >= 2 * YL) & (lanes < 2 * YL + 16), piece, value)
        bbuf[p] = value

    bcopies = [
        remote(bbuf.at[peer(pa, d)], mine48(brecv, pa), bsend_s.at[d], brecv_s.at[pa], {"pa": peer(pa, d)})
        for d in range(1, NB)
    ]
    for copy in bcopies:
        copy.start()
    brecv[pl.ds(pl.multiple_of(pa * YL, YL), YL), :] = bbuf[pa]

    rows = lax.broadcasted_iota(jnp.int32, (LANES, LANES), 0)
    scale[...] = jnp.where(
        rows < YL, a_of(0, (LANES, LANES)), jnp.where(rows < 2 * YL, b_of(ZL - 1, (LANES, LANES)), 1.0)
    )
    for copy in bcopies:
        copy.wait_send()

    @pl.when(is_solver)
    def _():
        for d in range(1, NB):
            g = peer(gz, d)
            remote(rbuf.at[g], rrecv.at[me_s], rsend_s.at[d], rrecv_s.at[me_s], {"gz": g}).wait_send()

    for d in range(1, NB):
        p = peer(pa, d)
        remote(bbuf.at[p], mine48(brecv, p), bsend_s.at[d], brecv_s.at[p], {"pa": p}).wait_recv()

    def again(c):
        cols = pl.ds(pl.multiple_of(c * LANES, LANES), LANES)
        x = jnp.transpose(brecv[cols, :]) * scale[...]
        add = table_by(mc[0], mc[1], x)
        solve(lambda z: fh[z, :, cols] + add[z * YL : (z + 1) * YL], eloc, cols, work)
        for z in range(ZL):
            a, b = cut(work[z, :, cols])
            u = dot(s48[...], jnp.concatenate([a, b, a], axis=0))
            a, b = cut(u)
            s_hi[z * YL : (z + 1) * YL, cols] = a
            s_lo[z * YL : (z + 1) * YL, cols] = b

    pl.loop(0, CH)(again)
    for n in range(3):
        cols = slice(n * 256, (n + 1) * 256)
        r = dot(s_hi[...], cos_r[0, :, cols]) + dot(s_lo[...], cos_r[0, :, cols])
        out[:, cols] = r + dot(s_hi[...], cos_r[1, :, cols])


def on_device(source, cell_width):
    t = tables()
    args = [jnp.asarray(t[name]) for name in TABLES]
    vmem = pl.BlockSpec(memory_space=pltpu.VMEM)
    v = pltpu.VMEM
    dma = pltpu.SemaphoreType.DMA
    line = (NB, 8, HALF)
    out = pl.pallas_call(
        kernel,
        out_shape=jax.ShapeDtypeStruct((ZL * YL, N), F32),
        in_specs=[vmem, pl.BlockSpec(memory_space=pltpu.SMEM)] + [vmem] * len(args),
        out_specs=vmem,
        scratch_shapes=[
            v((ZL * YL, N), BF16),
            v((ZL * YL, N), BF16),
            v((ZL, YL, N), F32),
            v((ZL, YL, N), F32),
            v((ZL, YL, N), F32),
            v((N, LANES), F32),
            v((NB, YL, LANES), F32),
            v((ZL, LANES), F32),
            v((NB, ZL, LANES), F32),
            v((NB * ZL, LANES), F32),
            v((NB * ZL, LANES), F32),
            v((2 * YL, N), F32),
            v((ZL, YL, N), F32),
            v((ZL, YL, N), F32),
            v((NS, 2, 8, HALF), F32),
            v((NB, 2, 8, HALF), F32),
            v((NB, 2, 8, HALF), F32),
            v((NS, 2, 8, HALF), F32),
        ]
        + [v(line, F32)] * 7
        + [
            v((NB, YL, LANES), F32),
            v((N, LANES), F32),
            v((LANES, LANES), F32),
        ]
        + [dma((NB,))] * 10,
        compiler_params=pltpu.CompilerParams(
            collective_id=0, has_side_effects=True, vmem_limit_bytes=60 * 1024 * 1024
        ),
        name="poisson",
    )(source.reshape(ZL * YL, N), cell_width, *args)
    return out.reshape(ZL, YL, N)


def solution(mesh):
    return jax.shard_map(
        on_device,
        mesh=mesh,
        in_specs=(P("gz", "pa", None), P("gz")),
        out_specs=P("gz", "pa", None),
        check_vma=False,
    )
```

```python
import functools

import jax
import jax.numpy as jnp
import numpy as np
from jax import lax
from jax.experimental import pallas as pl
from jax.experimental.pallas import tpu as pltpu
from jax.sharding import PartitionSpec as P

F32 = jnp.float32
BF16 = jnp.bfloat16
N = 768
NB = 16
ZL = 8
YL = 48
LANES = 128
CH = N // LANES
NC = 3
CW = N // NC
KB = CW // NB
IDLE = (0, 4, 10, 14)
SOLVERS = tuple(g for g in range(NB) if g not in IDLE)
NS = len(SOLVERS)


def split64(x):
    hi = x.astype(np.float32).astype(jnp.bfloat16)
    lo = (x - hi.astype(np.float64)).astype(np.float32).astype(jnp.bfloat16)
    return np.stack([hi, lo])


@functools.cache
def tables():
    n = np.arange(N)
    phases = n[:, None] * (2 * n[None, :] + 1) % (4 * N)
    weights = np.where(n == 0, np.sqrt(1.0 / N), np.sqrt(2.0 / N))
    cos_t = weights[:, None] * np.cos(phases * (np.pi / (2 * N)))

    def sine(width, rows, cols):
        p = rows[:, None] * cols[None, :] % (2 * (width + 1))
        return np.sqrt(2.0 / (width + 1)) * np.sin(p * (np.pi / (width + 1)))

    m = n + 1
    sin_t = sine(N, m, m)
    ml = np.arange(1, YL + 1)
    s48 = sine(YL, ml, ml)
    hi, lo = split64(s48)
    s48st = np.concatenate([hi, hi, lo], axis=1)
    mc = np.zeros((ZL * YL, LANES))
    mc[:YL, :YL] = s48
    mc[(ZL - 1) * YL :, YL : 2 * YL] = s48
    for z in range(ZL):
        mc[z * YL : (z + 1) * YL, 2 * YL + 2 * z] = s48[:, 0]
        mc[z * YL : (z + 1) * YL, 2 * YL + 2 * z + 1] = s48[:, YL - 1]
    own = np.zeros((NB, ZL, 2, N))
    beside = np.zeros((NB, ZL, 2, N))
    for p in range(NB):
        for e in range(2):
            row = YL * p + (YL - 1) * e
            own[p, :, e] = sin_t[row]
            near = row + (1 if e else -1)
            if 0 <= near < N:
                beside[p, :, e] = sin_t[near]
    own = own.reshape(2 * ZL * NB, N)
    beside = beside.reshape(2 * ZL * NB, N)
    lam_k = 4 * np.sin(n * np.pi / (2 * N)) ** 2
    lam_l = 4 * np.sin(m * np.pi / (2 * (N + 1))) ** 2
    lam_s = 4 * np.sin(ml * np.pi / (2 * (YL + 1))) ** 2
    rows = np.zeros((8, N), np.float32)
    rows[0] = lam_k
    rows[1] = lam_l
    cos2 = split64(cos_t)
    return dict(
        fwd=np.ascontiguousarray(cos2.reshape(2, NC, CW, N).transpose(1, 0, 3, 2)),
        bwd=np.ascontiguousarray(cos2.reshape(2, NC, CW, N).transpose(1, 0, 2, 3)),
        sin=split64(sin_t),
        s48=s48st,
        mct=split64(mc.T.copy()),
        mc=split64(mc),
        win=split64(own),
        wout=split64(beside.T.copy()),
        rows=rows,
        lam_s=np.broadcast_to(lam_s[:, None], (YL, CW)).astype(np.float32),
        lam_k=np.broadcast_to(lam_k[:, None], (N, LANES)).astype(np.float32).reshape(NC * NB, KB, LANES),
    )


TABLES = ("fwd", "bwd", "sin", "s48", "mct", "mc", "win", "wout", "rows", "lam_s", "lam_k")


def cut(x):
    hi = x.astype(BF16)
    return hi, (x - hi.astype(F32)).astype(BF16)


def dot(a, b):
    return jnp.dot(a, b, preferred_element_type=F32)


def by_table(a, b, hi, lo):
    return dot(a, hi) + dot(b, hi) + dot(a, lo)


def table_by(hi, lo, x):
    a, b = cut(x)
    return dot(hi, a) + dot(hi, b) + dot(lo, a)


def recip(x):
    return 1.0 / x


def remote(src, dst, send, recv, where):
    return pltpu.make_async_remote_copy(
        src_ref=src,
        dst_ref=dst,
        send_sem=send,
        recv_sem=recv,
        device_id=where,
        device_id_type=pl.DeviceIdType.MESH,
    )


def rolled(x, shift):
    shift %= LANES
    return x if shift == 0 else pltpu.roll(x, shift, axis=1)


def wide(row, like):
    return jnp.broadcast_to(jnp.concatenate([row] * (like[1] // LANES), axis=1), like)


def kernel(
    src_h, cw, fwd_h, bwd_h, sin_h, s48_h, mct_h, mc_h, win_h, wout_h, rows_h, lam_s_h, lam_k_h, out,
    src, fwd, bwd, sin_r, s48, mct, mc, win, wout, lam_rows, lam_s, lam_k,
    s_hi, s_lo, fh, work, eloc, pbuf, precv, wmine, widths, alpha, beta, r_before, r_after,
    rhy, eg, gwork, qbuf, qrecv, rbuf, rrecv, ks, ku0, ku7, kv0, kv7, kh, kia, kc, hh, ss, bbuf, brecv,
    load_s, psend_s, precv_s, wsend_s, wrecv_s, qsend_s, qrecv_s, rsend_s, rrecv_s, bsend_s, brecv_s,
):
    pa = lax.axis_index("pa")
    gz = lax.axis_index("gz")

    def peer(me, d):
        return lax.rem(me + d, NB)

    loads = {}

    def load(name, h, v):
        loads[name] = pltpu.make_async_copy(h, v, load_s.at[len(loads)])
        loads[name].start()

    def need(*names):
        for name in names:
            loads[name].wait()

    load("src", src_h, src)
    load("fwd0", fwd_h.at[0], fwd.at[0])
    load("s48", s48_h, s48)
    load("rows", rows_h, lam_rows)
    load("lam_s", lam_s_h, lam_s)
    load("mct", mct_h, mct)
    for c in range(NC):
        load("lam_k%d" % c, lam_k_h.at[NB * c + pa], lam_k.at[c])

    barrier = pltpu.get_barrier_semaphore()
    for d in range(1, NB):
        pl.semaphore_signal(barrier, inc=1, device_id={"pa": peer(pa, d)}, device_id_type=pl.DeviceIdType.MESH)
        pl.semaphore_signal(barrier, inc=1, device_id={"gz": peer(gz, d)}, device_id_type=pl.DeviceIdType.MESH)

    for z in range(ZL):
        wmine[z : z + 1, :] = jnp.full((1, LANES), cw[z], F32)
    w = wmine[...]
    at = lax.broadcasted_iota(jnp.int32, (ZL, LANES), 0)
    al_b = 2.0 / ((jnp.where(at == 0, w, pltpu.roll(w, 1, axis=0)) + w) * w)
    be_b = 2.0 / ((w + jnp.where(at == ZL - 1, w, pltpu.roll(w, ZL - 1, axis=0))) * w)

    def a_of(z, like):
        return wide(al_b[z : z + 1, :], like)

    def b_of(z, like):
        return wide(be_b[z : z + 1, :], like)

    def factor(e_ref, lam):
        like = lam.shape
        e = None
        for z in range(ZL):
            d = a_of(z, like) + b_of(z, like) + lam
            if z:
                d = d - a_of(z, like) * b_of(z - 1, like) * e
            e = recip(d)
            e_ref[z] = e

    def solve(rhs_of, e_ref, x_ref):
        like = x_ref.shape[1:]
        y = None
        for z in range(ZL):
            r = rhs_of(z)
            if z:
                r = r + a_of(z, like) * y
            y = e_ref[z] * r
            x_ref[z] = y
        last = y
        for z in range(ZL - 2, -1, -1):
            y = x_ref[z] + e_ref[z] * b_of(z, like) * y
            x_ref[z] = y
        return y, last

    need("src", "fwd0", "s48")
    load("fwd1", fwd_h.at[1], fwd.at[1])
    load("fwd2", fwd_h.at[2], fwd.at[2])
    s_hi[...], s_lo[...] = cut(src[...])

    def sines(x):
        a, b = cut(x)
        return dot(s48[...], jnp.concatenate([a, b, a], axis=0))

    def block(c):
        f = by_table(s_hi[...], s_lo[...], fwd[c, 0], fwd[c, 1])
        for z in range(ZL):
            fh[c, z] = sines(f[z * YL : (z + 1) * YL])
        if c == 0:
            need("rows", "lam_s", "mct")
        factor(eloc.at[c], lam_s[...] + lam_rows[0:1, c * CW : (c + 1) * CW])
        solve(lambda z: fh[c, z], eloc.at[c], work.at[c])
        p = table_by(mct[0], mct[1], work[c].reshape(ZL * YL, CW))
        for t in range(CW // LANES):
            cols = slice(t * LANES, (t + 1) * LANES)
            pbuf[c, cols, :] = jnp.transpose(p[:, cols])

    def mine(ref, c, q):
        return ref.at[c, pl.ds(pl.multiple_of(q * KB, KB), KB), :]

    copies = []

    def start(copy):
        copies.append(copy)
        copy.start()

    def send_perimeter(c):
        for d in range(1, NB):
            q = peer(pa, d)
            start(remote(mine(pbuf, c, q), precv.at[c, pa], psend_s.at[c, d], precv_s.at[c, pa], {"pa": q}))
        precv[c, pa] = pbuf[c, pl.ds(pl.multiple_of(pa * KB, KB), KB), :]

    for c in range(NC):
        if c:
            need("fwd%d" % c)
        block(c)
        if c == 0:
            load("win", win_h, win)
            load("sin", sin_h, sin_r)
            load("wout", wout_h, wout)
            load("mc", mc_h, mc)
            load("bwd", bwd_h, bwd)
            pl.semaphore_wait(barrier, 2 * (NB - 1))
        send_perimeter(c)
        if c == 0:
            for d in range(1, NB):
                start(remote(wmine, widths.at[gz], wsend_s.at[d], wrecv_s.at[gz], {"gz": peer(gz, d)}))
            widths[gz] = wmine[...]

    need(*("lam_k%d" % c for c in range(NC)))
    for c in range(NC):
        factor(eg.at[c], wide(lam_k[c], (KB, N)) + lam_rows[1:2, :])

    for d in range(1, NB):
        g = peer(gz, d)
        remote(wmine, widths.at[g], wsend_s.at[d], wrecv_s.at[g], {"gz": g}).wait_recv()
    w = widths[...].reshape(NB * ZL, LANES)
    at = lax.broadcasted_iota(jnp.int32, (NB * ZL, LANES), 0)
    before = jnp.where(at == 0, 0.0, pltpu.roll(w, 1, axis=0))
    after = jnp.where(at == NB * ZL - 1, 0.0, pltpu.roll(w, NB * ZL - 1, axis=0))
    alpha[...] = 2.0 / ((before + w) * w)
    beta[...] = 2.0 / ((w + after) * w)
    r_before[...] = (before - w) / (2.0 * w)
    r_after[...] = (after - w) / (2.0 * w)

    me_s = gz - sum(((gz > g).astype(jnp.int32) for g in IDLE), jnp.int32(0))
    is_solver = functools.reduce(lambda x, y: x & y, [gz != g for g in IDLE])
    line = (8 * NC, LANES)

    def row_of(ref, i):
        return jnp.broadcast_to(ref[pl.ds(i, 1), :], line)

    @pl.when(is_solver)
    def _():
        rt = lax.div(me_s, CH)
        lt = lax.rem(me_s, CH)
        lam = jnp.concatenate([lam_k[c, pl.ds(pl.multiple_of(8 * rt, 8), 8), :] for c in range(NC)], axis=0)
        lam = lam + lam_rows[1:2, pl.ds(pl.multiple_of(lt * LANES, LANES), LANES)]

        def coefficients(b, carry):
            al = [row_of(alpha, b * ZL + z) for z in range(ZL)]
            be = [row_of(beta, b * ZL + z) for z in range(ZL)]
            e = recip(al[0] + be[0] + lam)
            prod_e = e
            prod_b = be[0]
            for z in range(1, ZL):
                e = recip(al[z] + be[z] + lam - al[z] * be[z - 1] * e)
                prod_e = prod_e * e * al[z]
                prod_b = prod_b * be[z] / al[z]
            g = recip(al[ZL - 1] + be[ZL - 1] + lam)
            for z in range(ZL - 2, -1, -1):
                g = recip(al[z] + be[z] + lam - be[z] * al[z + 1] * g)
            kh[b] = g * al[0]
            ks[b] = prod_e * al[0]
            kia[b] = prod_e * prod_b
            kc[b] = e * be[ZL - 1]
            return carry

        lax.fori_loop(0, NB, coefficients, 0)
        c = jnp.zeros(line, F32)
        for b in range(NB):
            a00, a70, a07, a77 = kh[b], ks[b], kia[b], kc[b]
            inv = recip(1.0 - a00 * c)
            mixed = a70 * c * inv
            rb = row_of(r_before, b * ZL)
            ra = row_of(r_after, b * ZL + ZL - 1)
            p00 = 1.0 + a00 * rb
            p07 = a07 * ra
            ku0[b] = a70 * rb + mixed * p00
            ku7[b] = 1.0 + a77 * ra + mixed * p07
            kv0[b] = inv * p00
            kv7[b] = inv * p07
            ks[b] = a70 * inv
            kh[b] = a00 * inv
            kia[b] = a07 * inv
            c = a77 + mixed * a07
            kc[b] = c

    small = (KB, LANES)
    lanes = lax.broadcasted_iota(jnp.int32, small, 1)
    odd = lax.rem(lanes, 2) == 1
    at_z = [lax.div(lax.rem(lanes, 16), 2) == z for z in range(ZL)]
    zero = jnp.zeros(small, F32)
    near = {}

    def ends(c):
        for d in range(1, NB):
            p = peer(pa, d)
            remote(mine(pbuf, c, p), precv.at[c, p], psend_s.at[c, d], precv_s.at[c, p], {"pa": p}).wait_recv()

        def gathered(base, t):
            value = zero
            for p in range(NB):
                first = YL * p - LANES * t
                if first + YL <= 0 or first >= LANES:
                    continue
                piece = rolled(precv[c, p], first - base)
                value = jnp.where((lanes >= first) & (lanes < first + YL), piece, value)
            return value

        def beside(t):
            value = zero
            for p in range(8 * t, 8 * t + 8):
                at_p = lax.div(lanes, 16) == p - 8 * t
                first = 16 * (p - 8 * t) - 2 * YL
                if p > 0:
                    value = jnp.where(at_p & ~odd, rolled(precv[c, p - 1], first - 1), value)
                if p < NB - 1:
                    value = jnp.where(at_p & odd, rolled(precv[c, p + 1], first + 1), value)
            return value

        planes = jnp.concatenate(
            [jnp.concatenate([gathered(base, t) for t in range(CH)], axis=1) for base in (0, YL)], axis=0
        )
        near[c] = [beside(t) for t in range(2)]
        rows = jnp.concatenate(
            [jnp.concatenate([jnp.where(at_z[z], v, 0.0) for v in near[c]], axis=1) for z in range(ZL)], axis=0
        )
        if c == 0:
            need("win", "sin")
        rhy[c] = by_table(*cut(rows), win[0], win[1]).reshape(ZL, KB, N)
        v = by_table(*cut(planes), sin_r[0], sin_r[1])
        first, last = solve(lambda z: rhy[c, z], eg.at[c], gwork.at[c])
        q = (v[0:KB] + first, v[KB : 2 * KB] + last)
        for s in range(NS):
            rt, lt = divmod(s, CH)
            for i in range(2):
                qbuf[c, s, i] = q[i][8 * rt : 8 * rt + 8, lt * LANES : (lt + 1) * LANES]
        for s, g in enumerate(SOLVERS):

            @pl.when(gz != g)
            def _():
                remote(qbuf.at[c, s], qrecv.at[c, gz], qsend_s.at[c, s], qrecv_s.at[c, gz], {"gz": g}).start()

            @pl.when(gz == g)
            def _():
                qrecv[c, gz] = qbuf[c, s]

    def chain(c):
        for d in range(1, NB):
            g = peer(gz, d)
            remote(qbuf.at[c, 0], qrecv.at[c, g], qsend_s.at[c, 0], qrecv_s.at[c, g], {"gz": g}).wait_recv()
        part = slice(8 * c, 8 * c + 8)

        def row8(ref, i):
            return jnp.broadcast_to(ref[i : i + 1, :], (8, LANES))

        s = None
        for b in range(NB):
            q0, q7 = qrecv[c, b, 0], qrecv[c, b, 1]
            h = kv0[b, part] * q0 + kv7[b, part] * q7
            v = ku0[b, part] * q0 + ku7[b, part] * q7
            if b:
                h = h + kh[b, part] * s
                v = v + ks[b, part] * s
            s = v
            hh[b] = h
            ss[b] = s
        upper = None
        for b in range(NB - 1, -1, -1):
            head = hh[b]
            tail = ss[b]
            if b < NB - 1:
                head = head + kia[b, part] * upper
                tail = tail + kc[b, part] * upper
            hh[b] = head
            ss[b] = tail
            upper = head
        for b in range(NB):
            low = row8(r_before, b * ZL) * hh[b]
            if b:
                low = low + ss[b - 1]
            high = row8(r_after, b * ZL + ZL - 1) * ss[b]
            if b < NB - 1:
                high = high + hh[b + 1]
            rbuf[c, b, 0] = row8(alpha, b * ZL) * low
            rbuf[c, b, 1] = row8(beta, b * ZL + ZL - 1) * high
        for d in range(1, NB):
            g = peer(gz, d)
            remote(rbuf.at[c, g], rrecv.at[c, me_s], rsend_s.at[c, d], rrecv_s.at[c, me_s], {"gz": g}).start()
        rrecv[c, me_s] = rbuf[c, gz]

    def inner(c):
        for s, g in enumerate(SOLVERS):

            @pl.when(gz != g)
            def _():
                remote(qbuf.at[c, s], rrecv.at[c, s], qsend_s.at[c, s], rrecv_s.at[c, s], {"gz": g}).wait_recv()

        low, high = (
            jnp.concatenate(
                [jnp.concatenate([rrecv[c, CH * rt + lt, i] for lt in range(CH)], axis=1) for rt in range(2)], axis=0
            )
            for i in range(2)
        )
        ends_of = {0: low, ZL - 1: high}
        solve(lambda z: rhy[c, z] + ends_of[z] if z in ends_of else rhy[c, z], eg.at[c], gwork.at[c])
        if c == 0:
            need("wout")
        r = by_table(*cut(gwork[c].reshape(ZL * KB, N)), wout[0], wout[1])
        planes = by_table(*cut(jnp.concatenate([low, high], axis=0)), sin_r[0], sin_r[1])
        edge = []
        for t in range(2):
            value = near[c][t]
            for z in range(ZL):
                value = value + jnp.where(at_z[z], r[z * KB : (z + 1) * KB, t * LANES : (t + 1) * LANES], 0.0)
            edge.append(value)
        for p in range(NB):
            value = zero
            for e in range(2):
                for t in range(YL * p // LANES, (YL * p + YL - 1) // LANES + 1):
                    move = YL * e - YL * p
                    first = max(LANES * t, YL * p) + move
                    stop = min(LANES * (t + 1), YL * p + YL) + move
                    piece = rolled(planes[e * KB : (e + 1) * KB, t * LANES : (t + 1) * LANES], LANES * t + move)
                    value = jnp.where((lanes >= first) & (lanes < stop), piece, value)
            piece = rolled(edge[p // 8], 2 * YL - 16 * (p % 8))
            bbuf[c, p] = jnp.where((lanes >= 2 * YL) & (lanes < 2 * YL + 16), piece, value)
        for d in range(1, NB):
            p = peer(pa, d)
            start(remote(bbuf.at[c, p], mine(brecv, c, pa), bsend_s.at[c, d], brecv_s.at[c, pa], {"pa": p}))
        brecv[c, pl.ds(pl.multiple_of(pa * KB, KB), KB), :] = bbuf[c, pa]

    def again(c):
        for d in range(1, NB):
            p = peer(pa, d)
            remote(bbuf.at[c, p], mine(brecv, c, p), bsend_s.at[c, d], brecv_s.at[c, p], {"pa": p}).wait_recv()
        if c == 0:
            need("mc", "bwd")
        x = jnp.concatenate(
            [jnp.transpose(brecv[c, t * LANES : (t + 1) * LANES, :]) for t in range(CW // LANES)], axis=1
        )
        add = table_by(mc[0], mc[1], x)
        solve(lambda z: fh[c, z] + add[z * YL : (z + 1) * YL], eloc.at[c], work.at[c])
        u = jnp.concatenate([sines(work[c, z]) for z in range(ZL)], axis=0)
        part = by_table(*cut(u), bwd[c, 0], bwd[c, 1])
        if c == 0:
            out[...] = part
        else:
            out[...] += part

    for c in range(NC):
        ends(c)
    for c in range(NC):
        pl.when(is_solver)(functools.partial(chain, c))
    for c in range(NC):
        inner(c)
    for c in range(NC):
        again(c)

    for copy in copies:
        copy.wait_send()
    for c in range(NC):
        for s, g in enumerate(SOLVERS):

            @pl.when(gz != g)
            def _():
                remote(qbuf.at[c, s], qrecv.at[c, gz], qsend_s.at[c, s], qrecv_s.at[c, gz], {"gz": g}).wait_send()

        @pl.when(is_solver)
        def _():
            for d in range(1, NB):
                g = peer(gz, d)
                remote(rbuf.at[c, g], rrecv.at[c, me_s], rsend_s.at[c, d], rrecv_s.at[c, me_s], {"gz": g}).wait_send()


def on_device(source, cell_width):
    t = tables()
    args = [jnp.asarray(t[name]) for name in TABLES]
    hbm = pl.BlockSpec(memory_space=pltpu.HBM)
    v = pltpu.VMEM
    dma = pltpu.SemaphoreType.DMA
    here = [v(x.shape, x.dtype) for x in args[:-1]] + [v((NC, KB, LANES), F32)]
    coef = v((NB, 8 * NC, LANES), F32)
    out = pl.pallas_call(
        kernel,
        out_shape=jax.ShapeDtypeStruct((ZL * YL, N), F32),
        in_specs=[hbm, pl.BlockSpec(memory_space=pltpu.SMEM)] + [hbm] * len(args),
        out_specs=pl.BlockSpec(memory_space=pltpu.VMEM),
        scratch_shapes=[v((ZL * YL, N), F32)]
        + here
        + [
            v((ZL * YL, N), BF16),
            v((ZL * YL, N), BF16),
            v((NC, ZL, YL, CW), F32),
            v((NC, ZL, YL, CW), F32),
            v((NC, ZL, YL, CW), F32),
            v((NC, CW, LANES), F32),
            v((NC, NB, KB, LANES), F32),
            v((ZL, LANES), F32),
            v((NB, ZL, LANES), F32),
        ]
        + [v((NB * ZL, LANES), F32)] * 4
        + [
            v((NC, ZL, KB, N), F32),
            v((NC, ZL, KB, N), F32),
            v((NC, ZL, KB, N), F32),
            v((NC, NS, 2, 8, LANES), F32),
            v((NC, NB, 2, 8, LANES), F32),
            v((NC, NB, 2, 8, LANES), F32),
            v((NC, NS, 2, 8, LANES), F32),
        ]
        + [coef] * 8
        + [
            v((NB, 8, LANES), F32),
            v((NB, 8, LANES), F32),
            v((NC, NB, KB, LANES), F32),
            v((NC, CW, LANES), F32),
            dma((24,)),
            dma((NC, NB)),
            dma((NC, NB)),
            dma((NB,)),
            dma((NB,)),
        ]
        + [dma((NC, NB))] * 6,
        compiler_params=pltpu.CompilerParams(
            collective_id=0, has_side_effects=True, vmem_limit_bytes=44 * 1024 * 1024
        ),
        name="poisson",
    )(*(pltpu.with_memory_space_constraint(x, pltpu.HBM) for x in (source.reshape(ZL * YL, N), cell_width, *args)))
    return out.reshape(ZL, YL, N)


def solution(mesh):
    return jax.shard_map(
        on_device,
        mesh=mesh,
        in_specs=(P("gz", "pa", None), P("gz")),
        out_specs=P("gz", "pa", None),
        check_vma=False,
    )
```

```python
import functools

import jax
import jax.numpy as jnp
import numpy as np
from jax import lax
from jax.experimental import pallas as pl
from jax.experimental.pallas import tpu as pltpu
from jax.sharding import PartitionSpec as P

F32 = jnp.float32
BF16 = jnp.bfloat16
N = 768
NB = 16
ZL = 8
YL = 48
LANES = 128
CH = N // LANES
NC = 3
CW = N // NC
KB = CW // NB
IDLE = (0, 4, 10, 14)
PA_ORDER = (4, 12, 3, 5, 11, 13, 2, 6, 10, 14, 1, 7, 9, 15, 8)
GZ_ORDER = (12, 4, 11, 13, 5, 3, 10, 14, 6, 2, 7, 9, 8, 15, 1)
SOLVERS = tuple(g for g in range(NB) if g not in IDLE)
NS = len(SOLVERS)


def split64(x):
    hi = x.astype(np.float32).astype(jnp.bfloat16)
    lo = (x - hi.astype(np.float64)).astype(np.float32).astype(jnp.bfloat16)
    return np.stack([hi, lo])


@functools.cache
def tables():
    n = np.arange(N)
    phases = n[:, None] * (2 * n[None, :] + 1) % (4 * N)
    weights = np.where(n == 0, np.sqrt(1.0 / N), np.sqrt(2.0 / N))
    cos_t = weights[:, None] * np.cos(phases * (np.pi / (2 * N)))

    def sine(width, rows, cols):
        p = rows[:, None] * cols[None, :] % (2 * (width + 1))
        return np.sqrt(2.0 / (width + 1)) * np.sin(p * (np.pi / (width + 1)))

    m = n + 1
    sin_t = sine(N, m, m)
    ml = np.arange(1, YL + 1)
    s48 = sine(YL, ml, ml)
    hi, lo = split64(s48)
    s48st = np.concatenate([hi, hi, lo], axis=1)
    mc = np.zeros((ZL * YL, LANES))
    mc[:YL, :YL] = s48
    mc[(ZL - 1) * YL :, YL : 2 * YL] = s48
    for z in range(ZL):
        mc[z * YL : (z + 1) * YL, 2 * YL + 2 * z] = s48[:, 0]
        mc[z * YL : (z + 1) * YL, 2 * YL + 2 * z + 1] = s48[:, YL - 1]
    own = np.zeros((NB, ZL, 2, N))
    beside = np.zeros((NB, ZL, 2, N))
    for p in range(NB):
        for e in range(2):
            row = YL * p + (YL - 1) * e
            own[p, :, e] = sin_t[row]
            near = row + (1 if e else -1)
            if 0 <= near < N:
                beside[p, :, e] = sin_t[near]
    own = own.reshape(2 * ZL * NB, N)
    beside = beside.reshape(2 * ZL * NB, N)
    lam_k = 4 * np.sin(n * np.pi / (2 * N)) ** 2
    lam_l = 4 * np.sin(m * np.pi / (2 * (N + 1))) ** 2
    lam_s = 4 * np.sin(ml * np.pi / (2 * (YL + 1))) ** 2
    rows = np.zeros((8, N), np.float32)
    rows[0] = lam_k
    rows[1] = lam_l
    cos2 = split64(cos_t)
    return dict(
        fwd=np.ascontiguousarray(cos2.reshape(2, NC, CW, N).transpose(1, 0, 3, 2)),
        bwd=np.ascontiguousarray(cos2.reshape(2, NC, CW, N).transpose(1, 0, 2, 3)),
        sin=split64(sin_t),
        s48=s48st,
        mct=split64(mc.T.copy()).reshape(2 * LANES, ZL * YL),
        mc=split64(mc).reshape(2 * ZL * YL, LANES),
        win=split64(own),
        wout=split64(beside.T.copy()),
        rows=rows,
        lam_s=np.broadcast_to(lam_s[:, None], (YL, CW)).astype(np.float32),
        lam_k=np.broadcast_to(lam_k[:, None], (N, LANES)).astype(np.float32).reshape(NC * NB, KB, LANES),
    )


TABLES = ("fwd", "bwd", "sin", "s48", "mct", "mc", "win", "wout", "rows", "lam_s", "lam_k")


def cut(x):
    hi = x.astype(BF16)
    return hi, (x - hi.astype(F32)).astype(BF16)


def dot(a, b):
    return jnp.dot(a, b, preferred_element_type=F32)


def by_table(x, hi, lo):
    a, b = cut(x)
    m = x.shape[0]
    r = dot(jnp.concatenate([a, b], axis=0), hi)
    return r[:m] + r[m:] + dot(a, lo)


def table_by(t, x):
    a, b = cut(x)
    m = t.shape[0] // 2
    r = dot(t, a)
    return r[:m] + r[m:] + dot(t[:m], b)


def recip(x):
    return 1.0 / x


def remote(src, dst, send, recv, where):
    return pltpu.make_async_remote_copy(
        src_ref=src,
        dst_ref=dst,
        send_sem=send,
        recv_sem=recv,
        device_id=where,
        device_id_type=pl.DeviceIdType.MESH,
    )


def rolled(x, shift):
    shift %= LANES
    return x if shift == 0 else pltpu.roll(x, shift, axis=1)


def wide(row, like):
    return jnp.broadcast_to(jnp.concatenate([row] * (like[1] // LANES), axis=1), like)


def kernel(
    src_h, cw, fwd_h, bwd_h, sin_h, s48_h, mct_h, mc_h, win_h, wout_h, rows_h, lam_s_h, lam_k_h, out,
    src, fwd, bwd, sin_r, s48, mct, mc, win, wout, lam_rows, lam_s, lam_k,
    s_hi, s_lo, fh, work, eloc, pbuf, precv, wmine, widths, alpha, beta, r_before, r_after,
    rhy, eg, gwork, qbuf, qrecv, rbuf, rrecv, ks, ku0, ku7, kv0, kv7, kh, kia, kc, hh, ss, bbuf, brecv,
    load_s, send_s, recv_s, psend_s, precv_s, qsend_s, qrecv_s, rsend_s, rrecv_s, bsend_s, brecv_s,
):
    pa = lax.axis_index("pa")
    gz = lax.axis_index("gz")

    def peer(me, d):
        return lax.rem(me + d, NB)

    loads = {}

    def load(name, h, v):
        loads[name] = pltpu.make_async_copy(h, v, load_s.at[len(loads)])
        loads[name].start()

    def need(*names):
        for name in names:
            loads[name].wait()

    load("rows", rows_h, lam_rows)
    load("lam_s", lam_s_h, lam_s)
    load("src", src_h, src)
    load("fwd0", fwd_h.at[0], fwd.at[0])
    load("s48", s48_h, s48)
    load("mct", mct_h, mct)
    for c in range(NC):
        load("lam_k%d" % c, lam_k_h.at[NB * c + pa], lam_k.at[c])

    barrier = pltpu.get_barrier_semaphore()
    for d in range(1, NB):
        pl.semaphore_signal(barrier, inc=1, device_id={"pa": peer(pa, d)}, device_id_type=pl.DeviceIdType.MESH)
        pl.semaphore_signal(barrier, inc=1, device_id={"gz": peer(gz, d)}, device_id_type=pl.DeviceIdType.MESH)

    for z in range(ZL):
        wmine[z : z + 1, :] = jnp.full((1, LANES), cw[z], F32)
    w = wmine[...]
    at = lax.broadcasted_iota(jnp.int32, (ZL, LANES), 0)
    al_b = 2.0 / ((jnp.where(at == 0, w, pltpu.roll(w, 1, axis=0)) + w) * w)
    be_b = 2.0 / ((w + jnp.where(at == ZL - 1, w, pltpu.roll(w, ZL - 1, axis=0))) * w)

    def a_of(z, like):
        return wide(al_b[z : z + 1, :], like)

    def b_of(z, like):
        return wide(be_b[z : z + 1, :], like)

    def factor(e_ref, lam):
        like = lam.shape
        e = None
        for z in range(ZL):
            d = a_of(z, like) + b_of(z, like) + lam
            if z:
                d = d - a_of(z, like) * b_of(z - 1, like) * e
            e = recip(d)
            e_ref[z] = e

    def solve(rhs_of, e_ref, x_ref):
        like = x_ref.shape[1:]
        y = None
        for z in range(ZL):
            r = rhs_of(z)
            if z:
                r = r + a_of(z, like) * y
            y = e_ref[z] * r
            x_ref[z] = y
        last = y
        for z in range(ZL - 2, -1, -1):
            y = x_ref[z] + e_ref[z] * b_of(z, like) * y
            x_ref[z] = y
        return y, last

    need("rows", "lam_s")
    for c in range(NC):
        factor(eloc.at[c], lam_s[...] + lam_rows[0:1, c * CW : (c + 1) * CW])
    need("src", "fwd0", "s48")
    load("fwd1", fwd_h.at[1], fwd.at[1])
    load("fwd2", fwd_h.at[2], fwd.at[2])
    s_hi[...], s_lo[...] = cut(src[...])

    def sines(x):
        a, b = cut(x)
        return dot(s48[...], jnp.concatenate([a, b, a], axis=0))

    def block(c):
        f = dot(s_hi[...], fwd[c, 0]) + dot(s_lo[...], fwd[c, 0]) + dot(s_hi[...], fwd[c, 1])
        for z in range(ZL):
            fh[c, z] = sines(f[z * YL : (z + 1) * YL])
        if c == 0:
            need("mct")
        solve(lambda z: fh[c, z], eloc.at[c], work.at[c])
        p = table_by(mct[...], work[c].reshape(ZL * YL, CW))
        for t in range(CW // LANES):
            cols = slice(t * LANES, (t + 1) * LANES)
            pbuf[c, cols, :] = jnp.transpose(p[:, cols])

    def mine(ref, c, q):
        return ref.at[c, pl.ds(pl.multiple_of(q * KB, KB), KB), :]

    def wait_all(ref, sem):
        pltpu.make_async_copy(ref, ref, sem).wait()

    def send_perimeter(c):
        for d in PA_ORDER:
            q = peer(pa, d)
            remote(mine(pbuf, c, q), precv.at[c, pa], psend_s.at[c], precv_s.at[c], {"pa": q}).start()
        precv[c, pa] = pbuf[c, pl.ds(pl.multiple_of(pa * KB, KB), KB), :]

    for c in range(NC):
        if c:
            need("fwd%d" % c)
        block(c)
        if c == 0:
            load("win", win_h, win)
            load("sin", sin_h, sin_r)
            load("wout", wout_h, wout)
            load("mc", mc_h, mc)
            load("bwd", bwd_h, bwd)
            pl.semaphore_wait(barrier, 2 * (NB - 1))
        send_perimeter(c)
        if c == 0:
            for d in GZ_ORDER:
                remote(wmine, widths.at[gz], send_s.at[0], recv_s.at[0], {"gz": peer(gz, d)}).start()
            widths[gz] = wmine[...]

    need(*("lam_k%d" % c for c in range(NC)))
    for c in range(NC):
        factor(eg.at[c], wide(lam_k[c], (KB, N)) + lam_rows[1:2, :])

    wait_all(widths.at[0 : NB - 1], recv_s.at[0])
    w = widths[...].reshape(NB * ZL, LANES)
    at = lax.broadcasted_iota(jnp.int32, (NB * ZL, LANES), 0)
    before = jnp.where(at == 0, 0.0, pltpu.roll(w, 1, axis=0))
    after = jnp.where(at == NB * ZL - 1, 0.0, pltpu.roll(w, NB * ZL - 1, axis=0))
    alpha[...] = 2.0 / ((before + w) * w)
    beta[...] = 2.0 / ((w + after) * w)
    r_before[...] = (before - w) / (2.0 * w)
    r_after[...] = (after - w) / (2.0 * w)

    def place(g):
        return g - sum(((g > i).astype(jnp.int32) for i in IDLE), jnp.int32(0))

    def solves(g):
        return functools.reduce(lambda x, y: x & y, [g != i for i in IDLE])

    me_s = place(gz)
    is_solver = solves(gz)
    line = (8 * NC, LANES)

    def row_of(ref, i):
        return jnp.broadcast_to(ref[pl.ds(i, 1), :], line)

    @pl.when(is_solver)
    def _():
        rt = lax.div(me_s, CH)
        lt = lax.rem(me_s, CH)
        lam = jnp.concatenate([lam_k[c, pl.ds(pl.multiple_of(8 * rt, 8), 8), :] for c in range(NC)], axis=0)
        lam = lam + lam_rows[1:2, pl.ds(pl.multiple_of(lt * LANES, LANES), LANES)]

        def coefficients(b, carry):
            al = [row_of(alpha, b * ZL + z) for z in range(ZL)]
            be = [row_of(beta, b * ZL + z) for z in range(ZL)]
            e = recip(al[0] + be[0] + lam)
            prod_e = e
            prod_b = be[0]
            for z in range(1, ZL):
                e = recip(al[z] + be[z] + lam - al[z] * be[z - 1] * e)
                prod_e = prod_e * e * al[z]
                prod_b = prod_b * be[z] / al[z]
            g = recip(al[ZL - 1] + be[ZL - 1] + lam)
            for z in range(ZL - 2, -1, -1):
                g = recip(al[z] + be[z] + lam - be[z] * al[z + 1] * g)
            kh[b] = g * al[0]
            ks[b] = prod_e * al[0]
            kia[b] = prod_e * prod_b
            kc[b] = e * be[ZL - 1]
            return carry

        lax.fori_loop(0, NB, coefficients, 0)
        c = jnp.zeros(line, F32)
        for b in range(NB):
            a00, a70, a07, a77 = kh[b], ks[b], kia[b], kc[b]
            inv = recip(1.0 - a00 * c)
            mixed = a70 * c * inv
            rb = row_of(r_before, b * ZL)
            ra = row_of(r_after, b * ZL + ZL - 1)
            p00 = 1.0 + a00 * rb
            p07 = a07 * ra
            ku0[b] = a70 * rb + mixed * p00
            ku7[b] = 1.0 + a77 * ra + mixed * p07
            kv0[b] = inv * p00
            kv7[b] = inv * p07
            ks[b] = a70 * inv
            kh[b] = a00 * inv
            kia[b] = a07 * inv
            c = a77 + mixed * a07
            kc[b] = c

    small = (KB, LANES)
    lanes = lax.broadcasted_iota(jnp.int32, small, 1)
    odd = lax.rem(lanes, 2) == 1
    at_z = [lax.div(lax.rem(lanes, 16), 2) == z for z in range(ZL)]
    zero = jnp.zeros(small, F32)
    near = {}

    def ends(c):
        wait_all(precv.at[c, 0 : NB - 1], precv_s.at[c])

        def gathered(base, t):
            value = zero
            for p in range(NB):
                first = YL * p - LANES * t
                if first + YL <= 0 or first >= LANES:
                    continue
                piece = rolled(precv[c, p], first - base)
                value = jnp.where((lanes >= first) & (lanes < first + YL), piece, value)
            return value

        def beside(t):
            value = zero
            for p in range(8 * t, 8 * t + 8):
                at_p = lax.div(lanes, 16) == p - 8 * t
                first = 16 * (p - 8 * t) - 2 * YL
                if p > 0:
                    value = jnp.where(at_p & ~odd, rolled(precv[c, p - 1], first - 1), value)
                if p < NB - 1:
                    value = jnp.where(at_p & odd, rolled(precv[c, p + 1], first + 1), value)
            return value

        planes = jnp.concatenate(
            [jnp.concatenate([gathered(base, t) for t in range(CH)], axis=1) for base in (0, YL)], axis=0
        )
        near[c] = [beside(t) for t in range(2)]
        rows = jnp.concatenate(
            [jnp.concatenate([jnp.where(at_z[z], v, 0.0) for v in near[c]], axis=1) for z in range(ZL)], axis=0
        )
        if c == 0:
            need("win", "sin")
        rhy[c] = by_table(rows, win[0], win[1]).reshape(ZL, KB, N)
        v = by_table(planes, sin_r[0], sin_r[1])
        first, last = solve(lambda z: rhy[c, z], eg.at[c], gwork.at[c])
        q = (v[0:KB] + first, v[KB : 2 * KB] + last)
        for s in range(NS):
            rt, lt = divmod(s, CH)
            for i in range(2):
                qbuf[c, s, i] = q[i][8 * rt : 8 * rt + 8, lt * LANES : (lt + 1) * LANES]
        for d in GZ_ORDER:
            g = peer(gz, d)

            @pl.when(solves(g))
            def _():
                remote(qbuf.at[c, place(g)], qrecv.at[c, gz], qsend_s.at[c], qrecv_s.at[c], {"gz": g}).start()

        @pl.when(is_solver)
        def _():
            qrecv[c, gz] = qbuf[c, me_s]

    def chain(c):
        wait_all(qrecv.at[c, 0 : NB - 1], qrecv_s.at[c])
        part = slice(8 * c, 8 * c + 8)

        def row8(ref, i):
            return jnp.broadcast_to(ref[i : i + 1, :], (8, LANES))

        s = None
        for b in range(NB):
            q0, q7 = qrecv[c, b, 0], qrecv[c, b, 1]
            h = kv0[b, part] * q0 + kv7[b, part] * q7
            v = ku0[b, part] * q0 + ku7[b, part] * q7
            if b:
                h = h + kh[b, part] * s
                v = v + ks[b, part] * s
            s = v
            hh[b] = h
            ss[b] = s
        upper = None
        for b in range(NB - 1, -1, -1):
            head = hh[b]
            tail = ss[b]
            if b < NB - 1:
                head = head + kia[b, part] * upper
                tail = tail + kc[b, part] * upper
            hh[b] = head
            ss[b] = tail
            upper = head
        for b in range(NB):
            low = row8(r_before, b * ZL) * hh[b]
            if b:
                low = low + ss[b - 1]
            high = row8(r_after, b * ZL + ZL - 1) * ss[b]
            if b < NB - 1:
                high = high + hh[b + 1]
            rbuf[c, b, 0] = row8(alpha, b * ZL) * low
            rbuf[c, b, 1] = row8(beta, b * ZL + ZL - 1) * high
        for d in GZ_ORDER:
            g = peer(gz, d)
            remote(rbuf.at[c, g], rrecv.at[c, me_s], rsend_s.at[c], rrecv_s.at[c], {"gz": g}).start()
        rrecv[c, me_s] = rbuf[c, gz]

    def inner(c):
        @pl.when(is_solver)
        def _():
            wait_all(rrecv.at[c, 0 : NS - 1], rrecv_s.at[c])

        @pl.when(jnp.logical_not(is_solver))
        def _():
            wait_all(rrecv.at[c], rrecv_s.at[c])

        low, high = (
            jnp.concatenate(
                [jnp.concatenate([rrecv[c, CH * rt + lt, i] for lt in range(CH)], axis=1) for rt in range(2)], axis=0
            )
            for i in range(2)
        )
        ends_of = {0: low, ZL - 1: high}
        solve(lambda z: rhy[c, z] + ends_of[z] if z in ends_of else rhy[c, z], eg.at[c], gwork.at[c])
        if c == 0:
            need("wout")
        r = by_table((gwork[c].reshape(ZL * KB, N)), wout[0], wout[1])
        planes = by_table((jnp.concatenate([low, high], axis=0)), sin_r[0], sin_r[1])
        edge = []
        for t in range(2):
            value = near[c][t]
            for z in range(ZL):
                value = value + jnp.where(at_z[z], r[z * KB : (z + 1) * KB, t * LANES : (t + 1) * LANES], 0.0)
            edge.append(value)
        for p in range(NB):
            value = zero
            for e in range(2):
                for t in range(YL * p // LANES, (YL * p + YL - 1) // LANES + 1):
                    move = YL * e - YL * p
                    first = max(LANES * t, YL * p) + move
                    stop = min(LANES * (t + 1), YL * p + YL) + move
                    piece = rolled(planes[e * KB : (e + 1) * KB, t * LANES : (t + 1) * LANES], LANES * t + move)
                    value = jnp.where((lanes >= first) & (lanes < stop), piece, value)
            piece = rolled(edge[p // 8], 2 * YL - 16 * (p % 8))
            bbuf[c, p] = jnp.where((lanes >= 2 * YL) & (lanes < 2 * YL + 16), piece, value)
        for d in PA_ORDER:
            p = peer(pa, d)
            remote(bbuf.at[c, p], mine(brecv, c, pa), bsend_s.at[c], brecv_s.at[c], {"pa": p}).start()
        brecv[c, pl.ds(pl.multiple_of(pa * KB, KB), KB), :] = bbuf[c, pa]

    def again(c):
        wait_all(bbuf.at[c, 0 : NB - 1], brecv_s.at[c])
        if c == 0:
            need("mc", "bwd")
        x = jnp.concatenate(
            [jnp.transpose(brecv[c, t * LANES : (t + 1) * LANES, :]) for t in range(CW // LANES)], axis=1
        )
        add = table_by(mc[...], x)
        solve(lambda z: fh[c, z] + add[z * YL : (z + 1) * YL], eloc.at[c], work.at[c])
        u = jnp.concatenate([sines(work[c, z]) for z in range(ZL)], axis=0)
        part = by_table(u, bwd[c, 0], bwd[c, 1])
        if c == 0:
            out[...] = part
        else:
            out[...] += part

    for c in range(NC):
        ends(c)
    for c in range(NC):
        pl.when(is_solver)(functools.partial(chain, c))
    for c in range(NC):
        inner(c)
    for c in range(NC):
        again(c)

    wait_all(widths.at[0 : NB - 1], send_s.at[0])
    for c in range(NC):
        wait_all(precv.at[c, 0 : NB - 1], psend_s.at[c])
        wait_all(bbuf.at[c, 0 : NB - 1], bsend_s.at[c])

        @pl.when(jnp.logical_not(is_solver))
        def _():
            wait_all(qbuf.at[c], qsend_s.at[c])

        @pl.when(is_solver)
        def _():
            wait_all(qbuf.at[c, 0 : NS - 1], qsend_s.at[c])
            wait_all(rbuf.at[c, 0 : NB - 1], rsend_s.at[c])


def on_device(source, cell_width):
    t = tables()
    args = [jnp.asarray(t[name]) for name in TABLES]
    hbm = pl.BlockSpec(memory_space=pltpu.HBM)
    v = pltpu.VMEM
    dma = pltpu.SemaphoreType.DMA
    here = [v(x.shape, x.dtype) for x in args[:-1]] + [v((NC, KB, LANES), F32)]
    coef = v((NB, 8 * NC, LANES), F32)
    out = pl.pallas_call(
        kernel,
        out_shape=jax.ShapeDtypeStruct((ZL * YL, N), F32),
        in_specs=[hbm, pl.BlockSpec(memory_space=pltpu.SMEM)] + [hbm] * len(args),
        out_specs=pl.BlockSpec(memory_space=pltpu.VMEM),
        scratch_shapes=[v((ZL * YL, N), F32)]
        + here
        + [
            v((ZL * YL, N), BF16),
            v((ZL * YL, N), BF16),
            v((NC, ZL, YL, CW), F32),
            v((NC, ZL, YL, CW), F32),
            v((NC, ZL, YL, CW), F32),
            v((NC, CW, LANES), F32),
            v((NC, NB, KB, LANES), F32),
            v((ZL, LANES), F32),
            v((NB, ZL, LANES), F32),
        ]
        + [v((NB * ZL, LANES), F32)] * 4
        + [
            v((NC, ZL, KB, N), F32),
            v((NC, ZL, KB, N), F32),
            v((NC, ZL, KB, N), F32),
            v((NC, NS, 2, 8, LANES), F32),
            v((NC, NB, 2, 8, LANES), F32),
            v((NC, NB, 2, 8, LANES), F32),
            v((NC, NS, 2, 8, LANES), F32),
        ]
        + [coef] * 8
        + [
            v((NB, 8, LANES), F32),
            v((NB, 8, LANES), F32),
            v((NC, NB, KB, LANES), F32),
            v((NC, CW, LANES), F32),
            dma((16,)),
            dma((1,)),
            dma((1,)),
        ]
        + [dma((NC,))] * 8,
        compiler_params=pltpu.CompilerParams(
            collective_id=0, has_side_effects=True, vmem_limit_bytes=44 * 1024 * 1024
        ),
        name="poisson",
    )(*(pltpu.with_memory_space_constraint(x, pltpu.HBM) for x in (source.reshape(ZL * YL, N), cell_width, *args)))
    return out.reshape(ZL, YL, N)


def solution(mesh):
    return jax.shard_map(
        on_device,
        mesh=mesh,
        in_specs=(P("gz", "pa", None), P("gz")),
        out_specs=P("gz", "pa", None),
        check_vma=False,
    )
```

```python
import functools

import jax
import jax.numpy as jnp
import numpy as np
from jax import lax
from jax.experimental import pallas as pl
from jax.experimental.pallas import tpu as pltpu
from jax.sharding import PartitionSpec as P

F32 = jnp.float32
BF16 = jnp.bfloat16
N = 768
NB = 16
ZL = 8
YL = 48
LANES = 128
CH = N // LANES
NC = 3
CW = N // NC
KB = CW // NB
IDLE = (0, 4, 10, 14)
PA_ORDER = (4, 12, 3, 5, 11, 13, 2, 6, 10, 14, 1, 7, 9, 15, 8)
GZ_ORDER = (12, 4, 11, 13, 5, 3, 10, 14, 6, 2, 7, 9, 8, 15, 1)
SOLVERS = tuple(g for g in range(NB) if g not in IDLE)
NS = len(SOLVERS)


def split64(x):
    hi = x.astype(np.float32).astype(jnp.bfloat16)
    lo = (x - hi.astype(np.float64)).astype(np.float32).astype(jnp.bfloat16)
    return np.stack([hi, lo])


@functools.cache
def tables():
    n = np.arange(N)
    phases = n[:, None] * (2 * n[None, :] + 1) % (4 * N)
    weights = np.where(n == 0, np.sqrt(1.0 / N), np.sqrt(2.0 / N))
    cos_t = weights[:, None] * np.cos(phases * (np.pi / (2 * N)))

    def sine(width, rows, cols):
        p = rows[:, None] * cols[None, :] % (2 * (width + 1))
        return np.sqrt(2.0 / (width + 1)) * np.sin(p * (np.pi / (width + 1)))

    m = n + 1
    sin_t = sine(N, m, m)
    ml = np.arange(1, YL + 1)
    s48 = sine(YL, ml, ml)
    hi, lo = split64(s48)
    s48st = np.concatenate([hi, hi, lo], axis=1)
    mcp = np.zeros((2, ZL * YL, LANES // 2))
    mcp[0, :YL, :YL] = s48
    mcp[1, (ZL - 1) * YL :, :YL] = s48
    for z in range(ZL):
        mcp[:, z * YL : (z + 1) * YL, YL + 2 * z] = s48[:, 0]
        mcp[:, z * YL : (z + 1) * YL, YL + 2 * z + 1] = s48[:, YL - 1]
    own = np.zeros((NB, ZL, 2, N))
    beside = np.zeros((NB, ZL, 2, N))
    for p in range(NB):
        for e in range(2):
            row = YL * p + (YL - 1) * e
            own[p, :, e] = sin_t[row]
            near = row + (1 if e else -1)
            if 0 <= near < N:
                beside[p, :, e] = sin_t[near]
    own = own.reshape(2 * ZL * NB, N)
    beside = beside.reshape(2 * ZL * NB, N)
    lam_k = 4 * np.sin(n * np.pi / (2 * N)) ** 2
    lam_l = 4 * np.sin(m * np.pi / (2 * (N + 1))) ** 2
    lam_s = 4 * np.sin(ml * np.pi / (2 * (YL + 1))) ** 2
    rows = np.zeros((8, N), np.float32)
    rows[0] = lam_k
    rows[1] = lam_l
    cos2 = split64(cos_t)
    return dict(
        fwd=np.ascontiguousarray(cos2.reshape(2, NC, CW, N).transpose(1, 0, 3, 2)),
        bwd=np.ascontiguousarray(cos2.reshape(2, NC, CW, N).transpose(1, 0, 2, 3)),
        sin=split64(sin_t),
        s48=s48st,
        mct=split64(mcp.transpose(0, 2, 1).copy()).transpose(1, 0, 2, 3).reshape(2, LANES, ZL * YL),
        mc=split64(mcp).transpose(1, 0, 2, 3).reshape(2, 2 * ZL * YL, LANES // 2),
        win=split64(own),
        wout=split64(beside.T.copy()),
        rows=rows,
        lam_s=np.broadcast_to(lam_s[:, None], (YL, CW)).astype(np.float32),
        lam_k=np.broadcast_to(lam_k[:, None], (N, LANES)).astype(np.float32).reshape(NC * 2 * NB, 8, LANES),
    )


TABLES = ("fwd", "bwd", "sin", "s48", "mct", "mc", "win", "wout", "rows", "lam_s", "lam_k")


def cut(x):
    hi = x.astype(BF16)
    return hi, (x - hi.astype(F32)).astype(BF16)


def dot(a, b):
    return jnp.dot(a, b, preferred_element_type=F32)


def by_table(x, hi, lo):
    a, b = cut(x)
    m = x.shape[0]
    r = dot(jnp.concatenate([a, b], axis=0), hi)
    return r[:m] + r[m:] + dot(a, lo)


def table_by(t, x):
    a, b = cut(x)
    m = t.shape[0] // 2
    r = dot(t, a)
    return r[:m] + r[m:] + dot(t[:m], b)


def recip(x):
    return 1.0 / x


def remote(src, dst, send, recv, where):
    return pltpu.make_async_remote_copy(
        src_ref=src,
        dst_ref=dst,
        send_sem=send,
        recv_sem=recv,
        device_id=where,
        device_id_type=pl.DeviceIdType.MESH,
    )


def rolled(x, shift):
    shift %= LANES
    return x if shift == 0 else pltpu.roll(x, shift, axis=1)


def wide(row, like):
    return jnp.broadcast_to(jnp.concatenate([row] * (like[1] // LANES), axis=1), like)


def kernel(
    src_h, cw, fwd_h, bwd_h, sin_h, s48_h, mct_h, mc_h, win_h, wout_h, rows_h, lam_s_h, lam_k_h, out,
    src, fwd, bwd, sin_r, s48, mct, mc, win, wout, lam_rows, lam_s, lam_k,
    s_st, fh, work, eloc, pbuf, precv, wmine, wother, widths, alpha, beta, r_before, r_after,
    rhy, eg, gwork, qbuf, qrecv, rbuf, rrecv, ks, ku0, ku7, kv0, kv7, kh, kia, kc, hh, ss, bbuf, brecv,
    m_own, m_other, xbuf, xrecv,
    load_s, send_s, recv_s, psend_s, precv_s, qsend_s, qrecv_s, rsend_s, rrecv_s, bsend_s, brecv_s, xsend_s, xrecv_s,
):
    pa = lax.axis_index("pa")
    gz = lax.axis_index("gz")
    core = lax.rem(gz, 2)

    def peer(me, d):
        return lax.rem(me + d, NB)

    loads = {}

    def load(name, h, v):
        loads[name] = pltpu.make_async_copy(h, v, load_s.at[len(loads)])
        loads[name].start()

    def need(*names):
        for name in names:
            loads[name].wait()

    load("rows", rows_h, lam_rows)
    load("lam_s", lam_s_h, lam_s)
    load("src", src_h, src)
    load("fwd0", fwd_h.at[0], fwd.at[0])
    load("s48", s48_h, s48)
    load("mct", mct_h.at[core], mct)
    for c in range(NC):
        for h in range(2):
            load("lam_k%d" % (2 * c + h), lam_k_h.at[NB * (2 * c + h) + pa], lam_k.at[c, h])

    barrier = pltpu.get_barrier_semaphore()
    for d in range(1, NB):
        pl.semaphore_signal(barrier, inc=1, device_id={"pa": peer(pa, d)}, device_id_type=pl.DeviceIdType.MESH)
        pl.semaphore_signal(barrier, inc=1, device_id={"gz": peer(gz, d)}, device_id_type=pl.DeviceIdType.MESH)

    for z in range(ZL):
        wmine[z : z + 1, :] = jnp.full((1, LANES), cw[z], F32)
    def own_links(w):
        at = lax.broadcasted_iota(jnp.int32, (ZL, LANES), 0)
        al = 2.0 / ((jnp.where(at == 0, w, pltpu.roll(w, 1, axis=0)) + w) * w)
        be = 2.0 / ((w + jnp.where(at == ZL - 1, w, pltpu.roll(w, ZL - 1, axis=0))) * w)
        return al, be

    al_b, be_b = own_links(wmine[...])

    def a_of(z, like):
        return wide(al_b[z : z + 1, :], like)

    def b_of(z, like):
        return wide(be_b[z : z + 1, :], like)

    def factor(e_ref, lam):
        like = lam.shape
        e = None
        for z in range(ZL):
            d = a_of(z, like) + b_of(z, like) + lam
            if z:
                d = d - a_of(z, like) * b_of(z - 1, like) * e
            e = recip(d)
            e_ref[z] = e

    def solve(rhs_of, e_ref, x_ref):
        like = x_ref.shape[1:]
        y = None
        for z in range(ZL):
            r = rhs_of(z)
            if z:
                r = r + a_of(z, like) * y
            y = e_ref[z] * r
            x_ref[z] = y
        last = y
        for z in range(ZL - 2, -1, -1):
            y = x_ref[z] + e_ref[z] * b_of(z, like) * y
            x_ref[z] = y
        return y, last

    need("rows", "lam_s")
    for c in range(NC):
        factor(eloc.at[c], lam_s[...] + lam_rows[0:1, c * CW : (c + 1) * CW])
    need("src", "s48")
    load("fwd1", fwd_h.at[1], fwd.at[1])
    load("fwd2", fwd_h.at[2], fwd.at[2])
    s_st[0 : ZL * YL], s_st[ZL * YL :] = cut(src[...])

    def sines(x):
        a, b = cut(x)
        return dot(s48[...], jnp.concatenate([a, b, a], axis=0))

    def rows_of(q):
        return pl.ds(pl.multiple_of(q * 8, 8), 8)

    def wait_all(ref, sem):
        pltpu.make_async_copy(ref, ref, sem).wait()

    partner = {"gz": gz + 1 - 2 * core}

    def pair(c):
        w_o = wother[...]
        w_m = wmine[...]
        al_o, be_o = own_links(w_o)
        like = (YL, CW)

        def by_core(x, y):
            return jnp.where(core == 0, x, y)

        w_l, w_u = by_core(w_m, w_o), by_core(w_o, w_m)
        al_l, be_l = by_core(al_b, al_o), by_core(be_b, be_o)
        al_u, be_u = by_core(al_o, al_b), by_core(be_o, be_b)

        def row(x, z):
            return wide(x[z : z + 1, :], like)

        link_l = 2.0 / ((w_l[ZL - 1 : ZL] + w_u[0:1]) * w_l[ZL - 1 : ZL])
        link_u = 2.0 / ((w_l[ZL - 1 : ZL] + w_u[0:1]) * w_u[0:1])
        more_l = wide(be_l[ZL - 1 : ZL] - link_l, like)
        more_u = wide(al_u[0:1] - link_u, like)
        link_l = wide(link_l, like)
        link_u = wide(link_u, like)
        lam = lam_s[...] + lam_rows[0:1, c * CW : (c + 1) * CW]
        g_l = recip(row(al_l, 0) + row(be_l, 0) + lam)
        for z in range(1, ZL):
            g_l = recip(row(al_l, z) + row(be_l, z) + lam - row(al_l, z) * row(be_l, z - 1) * g_l)
        g_u = recip(row(al_u, ZL - 1) + row(be_u, ZL - 1) + lam)
        for z in range(ZL - 2, -1, -1):
            g_u = recip(row(al_u, z) + row(be_u, z) + lam - row(be_u, z) * row(al_u, z + 1) * g_u)
        rest_l = 1.0 - g_l * more_l
        rest_u = 1.0 - g_u * more_u
        inv = recip(rest_l * rest_u - g_l * g_u * link_l * link_u)
        own_l = link_l * link_u * g_u + more_l * rest_u
        own_u = link_l * link_u * g_l + more_u * rest_l
        m_own[c] = by_core(own_l, own_u) * inv
        m_other[c] = by_core(link_l, link_u) * inv

    def alone(c, i):
        first, last = solve(lambda z: fh[c, z], eloc.at[c], work.at[c])
        xbuf[i, c] = jnp.where(core == 0, last, first)

    def exchange(c, i):
        remote(xbuf.at[i, c], xrecv.at[i, c], xsend_s.at[i, c], xrecv_s.at[i, c], partner).start()

    def paired(c, i):
        wait_all(xrecv.at[i, c], xrecv_s.at[i, c])
        more = m_own[c] * xbuf[i, c] + m_other[c] * xrecv[i, c]
        ends_of = {0: jnp.where(core == 0, 0.0, more), ZL - 1: jnp.where(core == 0, more, 0.0)}
        solve(lambda z: fh[c, z] + ends_of[z] if z in ends_of else fh[c, z], eloc.at[c], work.at[c])

    def block(c):
        need("fwd%d" % c)
        f = dot(s_st[...], fwd[c, 0])
        f = f[: ZL * YL] + f[ZL * YL :] + dot(s_st[0 : ZL * YL], fwd[c, 1])
        for z in range(ZL):
            fh[c, z] = sines(f[z * YL : (z + 1) * YL])
        alone(c, 0)

    def perimeter(c):
        paired(c, 0)
        if c == 0:
            need("mct")
        p = table_by(mct[...], work[c].reshape(ZL * YL, CW))
        pbuf[c] = jnp.transpose(jnp.concatenate([p[:, :LANES], p[:, LANES:]], axis=0))
        for d in PA_ORDER:
            q = peer(pa, d)
            remote(pbuf.at[c, rows_of(q), :], precv.at[c, pa], psend_s.at[c], precv_s.at[c], {"pa": q}).start()
        precv[c, pa] = pbuf[c, rows_of(pa), :]

    block(0)
    load("win", win_h, win)
    load("sin", sin_h, sin_r)
    load("wout", wout_h, wout)
    load("mc", mc_h.at[core], mc)
    load("bwd", bwd_h, bwd)
    pl.semaphore_wait(barrier, 2 * (NB - 1))
    remote(wmine, wother, send_s.at[1], recv_s.at[1], partner).start()
    exchange(0, 0)
    for d in GZ_ORDER:
        remote(wmine, widths.at[gz], send_s.at[0], recv_s.at[0], {"gz": peer(gz, d)}).start()
    widths[gz] = wmine[...]
    block(1)
    exchange(1, 0)
    wait_all(wother, recv_s.at[1])
    pair(0)
    perimeter(0)
    block(2)
    exchange(2, 0)
    pair(1)
    perimeter(1)
    pair(2)
    perimeter(2)

    need(*("lam_k%d" % c for c in range(2 * NC)))
    for c in range(NC):
        factor(eg.at[c], wide(lam_k[c].reshape(KB, LANES), (KB, N)) + lam_rows[1:2, :])

    wait_all(widths.at[0 : NB - 1], recv_s.at[0])
    w = widths[...].reshape(NB * ZL, LANES)
    at = lax.broadcasted_iota(jnp.int32, (NB * ZL, LANES), 0)
    before = jnp.where(at == 0, 0.0, pltpu.roll(w, 1, axis=0))
    after = jnp.where(at == NB * ZL - 1, 0.0, pltpu.roll(w, NB * ZL - 1, axis=0))
    alpha[...] = 2.0 / ((before + w) * w)
    beta[...] = 2.0 / ((w + after) * w)
    r_before[...] = (before - w) / (2.0 * w)
    r_after[...] = (after - w) / (2.0 * w)

    def place(g):
        return g - sum(((g > i).astype(jnp.int32) for i in IDLE), jnp.int32(0))

    def solves(g):
        return functools.reduce(lambda x, y: x & y, [g != i for i in IDLE])

    me_s = place(gz)
    is_solver = solves(gz)
    line = (8 * NC, LANES)

    def row_of(ref, i):
        return jnp.broadcast_to(ref[pl.ds(i, 1), :], line)

    @pl.when(is_solver)
    def _():
        rt = lax.div(me_s, CH)
        lt = lax.rem(me_s, CH)
        lam = jnp.concatenate([lam_k[c, rt] for c in range(NC)], axis=0)
        lam = lam + lam_rows[1:2, pl.ds(pl.multiple_of(lt * LANES, LANES), LANES)]

        def coefficients(b, carry):
            al = [row_of(alpha, b * ZL + z) for z in range(ZL)]
            be = [row_of(beta, b * ZL + z) for z in range(ZL)]
            e = recip(al[0] + be[0] + lam)
            prod_e = e
            prod_b = be[0]
            for z in range(1, ZL):
                e = recip(al[z] + be[z] + lam - al[z] * be[z - 1] * e)
                prod_e = prod_e * e * al[z]
                prod_b = prod_b * be[z] / al[z]
            g = recip(al[ZL - 1] + be[ZL - 1] + lam)
            for z in range(ZL - 2, -1, -1):
                g = recip(al[z] + be[z] + lam - be[z] * al[z + 1] * g)
            kh[b] = g * al[0]
            ks[b] = prod_e * al[0]
            kia[b] = prod_e * prod_b
            kc[b] = e * be[ZL - 1]
            return carry

        lax.fori_loop(0, NB, coefficients, 0)
        c = jnp.zeros(line, F32)
        for b in range(NB):
            a00, a70, a07, a77 = kh[b], ks[b], kia[b], kc[b]
            inv = recip(1.0 - a00 * c)
            mixed = a70 * c * inv
            rb = row_of(r_before, b * ZL)
            ra = row_of(r_after, b * ZL + ZL - 1)
            p00 = 1.0 + a00 * rb
            p07 = a07 * ra
            ku0[b] = a70 * rb + mixed * p00
            ku7[b] = 1.0 + a77 * ra + mixed * p07
            kv0[b] = inv * p00
            kv7[b] = inv * p07
            ks[b] = a70 * inv
            kh[b] = a00 * inv
            kia[b] = a07 * inv
            c = a77 + mixed * a07
            kc[b] = c

    small = (KB, LANES)
    lanes = lax.broadcasted_iota(jnp.int32, small, 1)
    lane8 = lax.broadcasted_iota(jnp.int32, (8, LANES), 1)
    at_z = [lax.div(lax.rem(lanes, 16), 2) == z for z in range(ZL)]
    zero = jnp.zeros(small, F32)
    near = {}

    def ends(c):
        wait_all(precv.at[c, 0 : NB - 1], precv_s.at[c])

        tile8 = jnp.zeros((8, LANES), F32)
        odd = lax.rem(lane8, 2) == 1

        def gathered(h, t):
            value = tile8
            for p in range(NB):
                first = YL * p - LANES * t
                if first + YL <= 0 or first >= LANES:
                    continue
                piece = rolled(precv[c, p], first - LANES // 2 * h)
                value = jnp.where((lane8 >= first) & (lane8 < first + YL), piece, value)
            return value

        def beside(h, t):
            value = tile8
            for p in range(8 * t, 8 * t + 8):
                at_p = lax.div(lane8, 16) == p - 8 * t
                first = 16 * (p - 8 * t) - LANES // 2 * h - YL
                if p > 0:
                    value = jnp.where(at_p & ~odd, rolled(precv[c, p - 1], first - 1), value)
                if p < NB - 1:
                    value = jnp.where(at_p & odd, rolled(precv[c, p + 1], first + 1), value)
            return value

        planes = jnp.concatenate(
            [jnp.concatenate([gathered(h, t) for t in range(CH)], axis=1) for h in range(2)], axis=0
        )
        near[c] = [jnp.concatenate([beside(h, t) for h in range(2)], axis=0) for t in range(2)]
        rows = jnp.concatenate(
            [jnp.concatenate([jnp.where(at_z[z], v, 0.0) for v in near[c]], axis=1) for z in range(ZL)], axis=0
        )
        if c == 0:
            need("win", "sin")
        rhy[c] = by_table(rows, win[0], win[1]).reshape(ZL, KB, N)
        v = by_table(planes, sin_r[0], sin_r[1])
        first, last = solve(lambda z: rhy[c, z], eg.at[c], gwork.at[c])
        q = (first + jnp.where(core == 0, v, 0.0), last + jnp.where(core == 0, 0.0, v))
        for s in range(NS):
            rt, lt = divmod(s, CH)
            for i in range(2):
                qbuf[c, s, i] = q[i][8 * rt : 8 * rt + 8, lt * LANES : (lt + 1) * LANES]
        for d in GZ_ORDER:
            g = peer(gz, d)

            @pl.when(solves(g))
            def _():
                remote(qbuf.at[c, place(g)], qrecv.at[c, gz], qsend_s.at[c], qrecv_s.at[c], {"gz": g}).start()

        @pl.when(is_solver)
        def _():
            qrecv[c, gz] = qbuf[c, me_s]

    def chain(c):
        wait_all(qrecv.at[c, 0 : NB - 1], qrecv_s.at[c])
        part = slice(8 * c, 8 * c + 8)

        def row8(ref, i):
            return jnp.broadcast_to(ref[i : i + 1, :], (8, LANES))

        s = None
        for b in range(NB):
            q0, q7 = qrecv[c, b, 0], qrecv[c, b, 1]
            h = kv0[b, part] * q0 + kv7[b, part] * q7
            v = ku0[b, part] * q0 + ku7[b, part] * q7
            if b:
                h = h + kh[b, part] * s
                v = v + ks[b, part] * s
            s = v
            hh[b] = h
            ss[b] = s
        upper = None
        for b in range(NB - 1, -1, -1):
            head = hh[b]
            tail = ss[b]
            if b < NB - 1:
                head = head + kia[b, part] * upper
                tail = tail + kc[b, part] * upper
            hh[b] = head
            ss[b] = tail
            upper = head
        for b in range(NB):
            low = row8(r_before, b * ZL) * hh[b]
            if b:
                low = low + ss[b - 1]
            high = row8(r_after, b * ZL + ZL - 1) * ss[b]
            if b < NB - 1:
                high = high + hh[b + 1]
            rbuf[c, b, 0] = row8(alpha, b * ZL) * low
            rbuf[c, b, 1] = row8(beta, b * ZL + ZL - 1) * high
        for d in GZ_ORDER:
            g = peer(gz, d)
            remote(rbuf.at[c, g], rrecv.at[c, me_s], rsend_s.at[c], rrecv_s.at[c], {"gz": g}).start()
        rrecv[c, me_s] = rbuf[c, gz]

    def inner(c):
        @pl.when(is_solver)
        def _():
            wait_all(rrecv.at[c, 0 : NS - 1], rrecv_s.at[c])

        @pl.when(jnp.logical_not(is_solver))
        def _():
            wait_all(rrecv.at[c], rrecv_s.at[c])

        low, high = (
            jnp.concatenate(
                [jnp.concatenate([rrecv[c, CH * rt + lt, i] for lt in range(CH)], axis=1) for rt in range(2)], axis=0
            )
            for i in range(2)
        )
        ends_of = {0: low, ZL - 1: high}
        solve(lambda z: rhy[c, z] + ends_of[z] if z in ends_of else rhy[c, z], eg.at[c], gwork.at[c])
        if c == 0:
            need("wout")
        r = by_table((gwork[c].reshape(ZL * KB, N)), wout[0], wout[1])
        planes = by_table(jnp.where(core == 0, low, high), sin_r[0], sin_r[1])
        edge = []
        for t in range(2):
            value = near[c][t]
            for z in range(ZL):
                value = value + jnp.where(at_z[z], r[z * KB : (z + 1) * KB, t * LANES : (t + 1) * LANES], 0.0)
            edge.append(value)
        for p in range(NB):
            value = jnp.zeros((8, LANES), F32)
            for h in range(2):
                part = slice(8 * h, 8 * h + 8)
                base = h * LANES // 2
                for t in range(YL * p // LANES, (YL * p + YL - 1) // LANES + 1):
                    move = base - YL * p
                    first = max(LANES * t, YL * p) + move
                    stop = min(LANES * (t + 1), YL * p + YL) + move
                    piece = rolled(planes[part, t * LANES : (t + 1) * LANES], LANES * t + move)
                    value = jnp.where((lane8 >= first) & (lane8 < stop), piece, value)
                first = base + YL
                piece = rolled(edge[p // 8][part], first - 16 * (p % 8))
                value = jnp.where((lane8 >= first) & (lane8 < first + 16), piece, value)
            bbuf[c, p] = value
        for d in PA_ORDER:
            p = peer(pa, d)
            remote(bbuf.at[c, p], brecv.at[c, rows_of(pa), :], bsend_s.at[c], brecv_s.at[c], {"pa": p}).start()
        brecv[c, rows_of(pa), :] = bbuf[c, pa]

    def again(c):
        wait_all(bbuf.at[c, 0 : NB - 1], brecv_s.at[c])
        if c == 0:
            need("mc", "bwd")
        half = LANES // 2
        x = jnp.transpose(brecv[c])
        add = table_by(mc[...], jnp.concatenate([x[:half], x[half:]], axis=1))
        for z in range(ZL):
            fh[c, z] = fh[c, z] + add[z * YL : (z + 1) * YL]
        alone(c, 1)
        exchange(c, 1)

    def finish(c):
        paired(c, 1)
        u = jnp.concatenate([sines(work[c, z]) for z in range(ZL)], axis=0)
        part = by_table(u, bwd[c, 0], bwd[c, 1])
        if c == 0:
            out[...] = part
        else:
            out[...] += part

    for c in range(NC):
        ends(c)
    for c in range(NC):
        pl.when(is_solver)(functools.partial(chain, c))
    for c in range(NC):
        inner(c)
    again(0)
    again(1)
    finish(0)
    again(2)
    finish(1)
    finish(2)

    wait_all(widths.at[0 : NB - 1], send_s.at[0])
    wait_all(wother, send_s.at[1])
    for c in range(NC):
        wait_all(precv.at[c, 0 : NB - 1], psend_s.at[c])
        wait_all(bbuf.at[c, 0 : NB - 1], bsend_s.at[c])
        for i in range(2):
            wait_all(xbuf.at[i, c], xsend_s.at[i, c])

        @pl.when(jnp.logical_not(is_solver))
        def _():
            wait_all(qbuf.at[c], qsend_s.at[c])

        @pl.when(is_solver)
        def _():
            wait_all(qbuf.at[c, 0 : NS - 1], qsend_s.at[c])
            wait_all(rbuf.at[c, 0 : NB - 1], rsend_s.at[c])


def on_device(source, cell_width):
    t = tables()
    args = [jnp.asarray(t[name]) for name in TABLES]
    hbm = pl.BlockSpec(memory_space=pltpu.HBM)
    v = pltpu.VMEM
    dma = pltpu.SemaphoreType.DMA
    here = [v(x.shape[1:] if n in ("mc", "mct") else x.shape, x.dtype) for n, x in zip(TABLES[:-1], args)] + [v((NC, 2, 8, LANES), F32)]
    coef = v((NB, 8 * NC, LANES), F32)
    out = pl.pallas_call(
        kernel,
        out_shape=jax.ShapeDtypeStruct((ZL * YL, N), F32),
        in_specs=[hbm, pl.BlockSpec(memory_space=pltpu.SMEM)] + [hbm] * len(args),
        out_specs=pl.BlockSpec(memory_space=pltpu.VMEM),
        scratch_shapes=[v((ZL * YL, N), F32)]
        + here
        + [
            v((2 * ZL * YL, N), BF16),
            v((NC, ZL, YL, CW), F32),
            v((NC, ZL, YL, CW), F32),
            v((NC, ZL, YL, CW), F32),
            v((NC, LANES, LANES), F32),
            v((NC, NB, 8, LANES), F32),
            v((ZL, LANES), F32),
            v((ZL, LANES), F32),
            v((NB, ZL, LANES), F32),
        ]
        + [v((NB * ZL, LANES), F32)] * 4
        + [
            v((NC, ZL, KB, N), F32),
            v((NC, ZL, KB, N), F32),
            v((NC, ZL, KB, N), F32),
            v((NC, NS, 2, 8, LANES), F32),
            v((NC, NB, 2, 8, LANES), F32),
            v((NC, NB, 2, 8, LANES), F32),
            v((NC, NS, 2, 8, LANES), F32),
        ]
        + [coef] * 8
        + [
            v((NB, 8, LANES), F32),
            v((NB, 8, LANES), F32),
            v((NC, NB, 8, LANES), F32),
            v((NC, LANES, LANES), F32),
        ]
        + [v((NC, YL, CW), F32)] * 2
        + [v((2, NC, YL, CW), F32)] * 2
        + [
            dma((24,)),
            dma((2,)),
            dma((2,)),
        ]
        + [dma((NC,))] * 8
        + [dma((2, NC))] * 2,
        compiler_params=pltpu.CompilerParams(
            collective_id=0, has_side_effects=True, vmem_limit_bytes=44 * 1024 * 1024
        ),
        name="poisson",
    )(*(pltpu.with_memory_space_constraint(x, pltpu.HBM) for x in (source.reshape(ZL * YL, N), cell_width, *args)))
    return out.reshape(ZL, YL, N)


def solution(mesh):
    return jax.shard_map(
        on_device,
        mesh=mesh,
        in_specs=(P("gz", "pa", None), P("gz")),
        out_specs=P("gz", "pa", None),
        check_vma=False,
    )
```

```python
import functools

import jax
import jax.numpy as jnp
import numpy as np
from jax import lax
from jax.experimental import pallas as pl
from jax.experimental.pallas import tpu as pltpu
from jax.sharding import PartitionSpec as P

F32 = jnp.float32
BF16 = jnp.bfloat16
N = 768
NB = 16
ZL = 8
YL = 48
LANES = 128
CH = N // LANES
NC = 3
CW = N // NC
KB = CW // NB
IDLE = (0, 4, 10, 14)
PA_ORDER = (4, 12, 3, 5, 11, 13, 2, 6, 10, 14, 1, 7, 9, 15, 8)
GZ_ORDER = (12, 4, 11, 13, 5, 3, 10, 14, 6, 2, 7, 9, 8, 15, 1)
SOLVERS = tuple(g for g in range(NB) if g not in IDLE)
NS = len(SOLVERS)


def split64(x):
    hi = x.astype(np.float32).astype(jnp.bfloat16)
    lo = (x - hi.astype(np.float64)).astype(np.float32).astype(jnp.bfloat16)
    return np.stack([hi, lo])


@functools.cache
def tables():
    n = np.arange(N)
    phases = n[:, None] * (2 * n[None, :] + 1) % (4 * N)
    weights = np.where(n == 0, np.sqrt(1.0 / N), np.sqrt(2.0 / N))
    cos_t = weights[:, None] * np.cos(phases * (np.pi / (2 * N)))

    def sine(width, rows, cols):
        p = rows[:, None] * cols[None, :] % (2 * (width + 1))
        return np.sqrt(2.0 / (width + 1)) * np.sin(p * (np.pi / (width + 1)))

    m = n + 1
    sin_t = sine(N, m, m)
    ml = np.arange(1, YL + 1)
    s48 = sine(YL, ml, ml)
    hi, lo = split64(s48)
    s48st = np.concatenate([hi, hi, lo], axis=1)
    mcp = np.zeros((2, ZL * YL, LANES // 2))
    mcp[0, :YL, :YL] = s48
    mcp[1, (ZL - 1) * YL :, :YL] = s48
    for z in range(ZL):
        mcp[:, z * YL : (z + 1) * YL, YL + 2 * z] = s48[:, 0]
        mcp[:, z * YL : (z + 1) * YL, YL + 2 * z + 1] = s48[:, YL - 1]
    own = np.zeros((NB, ZL, 2, N))
    beside = np.zeros((NB, ZL, 2, N))
    for p in range(NB):
        for e in range(2):
            row = YL * p + (YL - 1) * e
            own[p, :, e] = sin_t[row]
            near = row + (1 if e else -1)
            if 0 <= near < N:
                beside[p, :, e] = sin_t[near]
    own = own.reshape(2 * ZL * NB, N)
    beside = beside.reshape(2 * ZL * NB, N)
    lam_k = 4 * np.sin(n * np.pi / (2 * N)) ** 2
    lam_l = 4 * np.sin(m * np.pi / (2 * (N + 1))) ** 2
    lam_s = 4 * np.sin(ml * np.pi / (2 * (YL + 1))) ** 2
    rows = np.zeros((8, N), np.float32)
    rows[0] = lam_k
    rows[1] = lam_l
    cos2 = split64(cos_t)
    return dict(
        fwd=np.ascontiguousarray(cos2.reshape(2, NC, CW, N).transpose(1, 0, 3, 2)),
        bwd=cos2,
        sin=split64(sin_t),
        s48=s48st,
        mct=split64(mcp.transpose(0, 2, 1).copy()).transpose(1, 0, 2, 3).reshape(2, LANES, ZL * YL),
        mc=np.concatenate([split64(mcp)[i] for i in (0, 0, 1)], axis=2),
        win=split64(own),
        wout=split64(beside.T.copy()),
        rows=rows,
        lam_s=np.broadcast_to(lam_s[:, None], (YL, CW)).astype(np.float32),
        lam_k=np.broadcast_to(lam_k[:, None], (N, LANES)).astype(np.float32).reshape(NC * 2 * NB, 8, LANES),
    )


TABLES = ("fwd", "bwd", "sin", "s48", "mct", "mc", "win", "wout", "rows", "lam_s", "lam_k")


def cut(x):
    hi = x.astype(BF16)
    return hi, (x - hi.astype(F32)).astype(BF16)


def dot(a, b):
    return jnp.dot(a, b, preferred_element_type=F32)


def by_table(x, hi, lo):
    a, b = cut(x)
    m = x.shape[0]
    r = dot(jnp.concatenate([a, b], axis=0), hi)
    return r[:m] + r[m:] + dot(a, lo)


def stacked(a, b, hi, lo):
    return dot(jnp.concatenate([a, b, a], axis=1), jnp.concatenate([hi, hi, lo], axis=0))


def table_by(t, x):
    a, b = cut(x)
    m = t.shape[0] // 2
    r = dot(t, a)
    return r[:m] + r[m:] + dot(t[:m], b)


def recip(x):
    return 1.0 / x


def remote(src, dst, send, recv, where):
    return pltpu.make_async_remote_copy(
        src_ref=src,
        dst_ref=dst,
        send_sem=send,
        recv_sem=recv,
        device_id=where,
        device_id_type=pl.DeviceIdType.MESH,
    )


def rolled(x, shift):
    shift %= LANES
    return x if shift == 0 else pltpu.roll(x, shift, axis=1)


def wide(row, like):
    return jnp.broadcast_to(jnp.concatenate([row] * (like[1] // LANES), axis=1), like)


def kernel(
    src_h, cw, fwd_h, bwd_h, sin_h, s48_h, mct_h, mc_h, win_h, wout_h, rows_h, lam_s_h, lam_k_h, out,
    src, fwd, bwd, sin_r, s48, mct, mc, win, wout, lam_rows, lam_s, lam_k,
    s_st, fh, work, eloc, pbuf, precv, wmine, wother, widths, alpha, beta, r_before, r_after,
    rhy, eg, gwork, qbuf, qrecv, rbuf, rrecv, ks, ku0, ku7, kv0, kv7, kh, kia, kc, hh, ss, bbuf, brecv,
    m_own, m_other, xbuf, xrecv,
    load_s, send_s, recv_s, psend_s, precv_s, qsend_s, qrecv_s, rsend_s, rrecv_s, bsend_s, brecv_s, xsend_s, xrecv_s,
):
    pa = lax.axis_index("pa")
    gz = lax.axis_index("gz")
    core = lax.rem(gz, 2)

    def peer(me, d):
        return lax.rem(me + d, NB)

    loads = {}

    def load(name, h, v):
        loads[name] = pltpu.make_async_copy(h, v, load_s.at[len(loads)])
        loads[name].start()

    def need(*names):
        for name in names:
            loads[name].wait()

    load("rows", rows_h, lam_rows)
    load("lam_s", lam_s_h, lam_s)
    load("src", src_h, src)
    load("fwd0", fwd_h.at[0], fwd.at[0])
    load("s48", s48_h, s48)
    load("mct", mct_h.at[core], mct)
    for c in range(NC):
        for h in range(2):
            load("lam_k%d" % (2 * c + h), lam_k_h.at[NB * (2 * c + h) + pa], lam_k.at[c, h])

    barrier = pltpu.get_barrier_semaphore()
    for d in range(1, NB):
        pl.semaphore_signal(barrier, inc=1, device_id={"pa": peer(pa, d)}, device_id_type=pl.DeviceIdType.MESH)
        pl.semaphore_signal(barrier, inc=1, device_id={"gz": peer(gz, d)}, device_id_type=pl.DeviceIdType.MESH)

    for z in range(ZL):
        wmine[z : z + 1, :] = jnp.full((1, LANES), cw[z], F32)
    def own_links(w):
        at = lax.broadcasted_iota(jnp.int32, (ZL, LANES), 0)
        al = 2.0 / ((jnp.where(at == 0, w, pltpu.roll(w, 1, axis=0)) + w) * w)
        be = 2.0 / ((w + jnp.where(at == ZL - 1, w, pltpu.roll(w, ZL - 1, axis=0))) * w)
        return al, be

    al_b, be_b = own_links(wmine[...])

    def a_of(z, like):
        return wide(al_b[z : z + 1, :], like)

    def b_of(z, like):
        return wide(be_b[z : z + 1, :], like)

    def factor(e_ref, lam):
        like = lam.shape
        e = None
        for z in range(ZL):
            d = a_of(z, like) + b_of(z, like) + lam
            if z:
                d = d - a_of(z, like) * b_of(z - 1, like) * e
            e = recip(d)
            e_ref[z] = e

    def solve(rhs_of, e_ref, x_ref):
        like = x_ref.shape[1:]
        y = None
        for z in range(ZL):
            r = rhs_of(z)
            if z:
                r = r + a_of(z, like) * y
            y = e_ref[z] * r
            x_ref[z] = y
        last = y
        for z in range(ZL - 2, -1, -1):
            y = x_ref[z] + e_ref[z] * b_of(z, like) * y
            x_ref[z] = y
        return y, last

    need("rows", "lam_s")
    for c in range(NC):
        factor(eloc.at[c], lam_s[...] + lam_rows[0:1, c * CW : (c + 1) * CW])
    need("src", "s48")
    load("fwd1", fwd_h.at[1], fwd.at[1])
    load("fwd2", fwd_h.at[2], fwd.at[2])
    s_st[0 : ZL * YL], s_st[ZL * YL :] = cut(src[...])

    def sines(x):
        a, b = cut(x)
        return dot(s48[...], jnp.concatenate([a, b, a], axis=0))

    def rows_of(q):
        return pl.ds(pl.multiple_of(q * 8, 8), 8)

    def wait_all(ref, sem):
        pltpu.make_async_copy(ref, ref, sem).wait()

    partner = {"gz": gz + 1 - 2 * core}

    def pair(c):
        w_o = wother[...]
        w_m = wmine[...]
        al_o, be_o = own_links(w_o)
        like = (YL, CW)

        def by_core(x, y):
            return jnp.where(core == 0, x, y)

        w_l, w_u = by_core(w_m, w_o), by_core(w_o, w_m)
        al_l, be_l = by_core(al_b, al_o), by_core(be_b, be_o)
        al_u, be_u = by_core(al_o, al_b), by_core(be_o, be_b)

        def row(x, z):
            return wide(x[z : z + 1, :], like)

        link_l = 2.0 / ((w_l[ZL - 1 : ZL] + w_u[0:1]) * w_l[ZL - 1 : ZL])
        link_u = 2.0 / ((w_l[ZL - 1 : ZL] + w_u[0:1]) * w_u[0:1])
        more_l = wide(be_l[ZL - 1 : ZL] - link_l, like)
        more_u = wide(al_u[0:1] - link_u, like)
        link_l = wide(link_l, like)
        link_u = wide(link_u, like)
        lam = lam_s[...] + lam_rows[0:1, c * CW : (c + 1) * CW]
        g_l = recip(row(al_l, 0) + row(be_l, 0) + lam)
        for z in range(1, ZL):
            g_l = recip(row(al_l, z) + row(be_l, z) + lam - row(al_l, z) * row(be_l, z - 1) * g_l)
        g_u = recip(row(al_u, ZL - 1) + row(be_u, ZL - 1) + lam)
        for z in range(ZL - 2, -1, -1):
            g_u = recip(row(al_u, z) + row(be_u, z) + lam - row(be_u, z) * row(al_u, z + 1) * g_u)
        rest_l = 1.0 - g_l * more_l
        rest_u = 1.0 - g_u * more_u
        inv = recip(rest_l * rest_u - g_l * g_u * link_l * link_u)
        own_l = link_l * link_u * g_u + more_l * rest_u
        own_u = link_l * link_u * g_l + more_u * rest_l
        m_own[c] = by_core(own_l, own_u) * inv
        m_other[c] = by_core(link_l, link_u) * inv

    def alone(c, i):
        first, last = solve(lambda z: fh[c, z], eloc.at[c], work.at[c])
        xbuf[i, c] = jnp.where(core == 0, last, first)

    def exchange(c, i):
        remote(xbuf.at[i, c], xrecv.at[i, c], xsend_s.at[i, c], xrecv_s.at[i, c], partner).start()

    def paired(c, i):
        wait_all(xrecv.at[i, c], xrecv_s.at[i, c])
        more = m_own[c] * xbuf[i, c] + m_other[c] * xrecv[i, c]
        ends_of = {0: jnp.where(core == 0, 0.0, more), ZL - 1: jnp.where(core == 0, more, 0.0)}
        solve(lambda z: fh[c, z] + ends_of[z] if z in ends_of else fh[c, z], eloc.at[c], work.at[c])

    def block(c):
        need("fwd%d" % c)
        f = dot(s_st[...], fwd[c, 0])
        f = f[: ZL * YL] + f[ZL * YL :] + dot(s_st[0 : ZL * YL], fwd[c, 1])
        for z in range(ZL):
            fh[c, z] = sines(f[z * YL : (z + 1) * YL])
        alone(c, 0)

    def perimeter(c):
        paired(c, 0)
        if c == 0:
            need("mct")
        p = table_by(mct[...], work[c].reshape(ZL * YL, CW))
        pbuf[c] = jnp.transpose(jnp.concatenate([p[:, :LANES], p[:, LANES:]], axis=0))
        for d in PA_ORDER:
            q = peer(pa, d)
            remote(pbuf.at[c, rows_of(q), :], precv.at[c, pa], psend_s.at[c], precv_s.at[c], {"pa": q}).start()
        precv[c, pa] = pbuf[c, rows_of(pa), :]

    block(0)
    load("win", win_h, win)
    load("sin", sin_h, sin_r)
    load("wout", wout_h, wout)
    load("mc", mc_h.at[core], mc)
    load("bwd", bwd_h, bwd)
    pl.semaphore_wait(barrier, 2 * (NB - 1))
    remote(wmine, wother, send_s.at[1], recv_s.at[1], partner).start()
    exchange(0, 0)
    for d in GZ_ORDER:
        remote(wmine, widths.at[gz], send_s.at[0], recv_s.at[0], {"gz": peer(gz, d)}).start()
    widths[gz] = wmine[...]
    block(1)
    exchange(1, 0)
    wait_all(wother, recv_s.at[1])
    pair(0)
    perimeter(0)
    block(2)
    exchange(2, 0)
    pair(1)
    perimeter(1)
    pair(2)
    perimeter(2)

    need(*("lam_k%d" % c for c in range(2 * NC)))
    for c in range(NC):
        factor(eg.at[c], wide(lam_k[c].reshape(KB, LANES), (KB, N)) + lam_rows[1:2, :])

    wait_all(widths.at[0 : NB - 1], recv_s.at[0])
    w = widths[...].reshape(NB * ZL, LANES)
    at = lax.broadcasted_iota(jnp.int32, (NB * ZL, LANES), 0)
    before = jnp.where(at == 0, 0.0, pltpu.roll(w, 1, axis=0))
    after = jnp.where(at == NB * ZL - 1, 0.0, pltpu.roll(w, NB * ZL - 1, axis=0))
    alpha[...] = 2.0 / ((before + w) * w)
    beta[...] = 2.0 / ((w + after) * w)
    r_before[...] = (before - w) / (2.0 * w)
    r_after[...] = (after - w) / (2.0 * w)

    def place(g):
        return g - sum(((g > i).astype(jnp.int32) for i in IDLE), jnp.int32(0))

    def solves(g):
        return functools.reduce(lambda x, y: x & y, [g != i for i in IDLE])

    me_s = place(gz)
    is_solver = solves(gz)
    line = (8 * NC, LANES)

    def row_of(ref, i):
        return jnp.broadcast_to(ref[pl.ds(i, 1), :], line)

    @pl.when(is_solver)
    def _():
        rt = lax.div(me_s, CH)
        lt = lax.rem(me_s, CH)
        lam = jnp.concatenate([lam_k[c, rt] for c in range(NC)], axis=0)
        lam = lam + lam_rows[1:2, pl.ds(pl.multiple_of(lt * LANES, LANES), LANES)]

        def coefficients(b, carry):
            al = [row_of(alpha, b * ZL + z) for z in range(ZL)]
            be = [row_of(beta, b * ZL + z) for z in range(ZL)]
            e = recip(al[0] + be[0] + lam)
            prod_e = e
            prod_b = be[0]
            for z in range(1, ZL):
                e = recip(al[z] + be[z] + lam - al[z] * be[z - 1] * e)
                prod_e = prod_e * e * al[z]
                prod_b = prod_b * be[z] / al[z]
            g = recip(al[ZL - 1] + be[ZL - 1] + lam)
            for z in range(ZL - 2, -1, -1):
                g = recip(al[z] + be[z] + lam - be[z] * al[z + 1] * g)
            kh[b] = g * al[0]
            ks[b] = prod_e * al[0]
            kia[b] = prod_e * prod_b
            kc[b] = e * be[ZL - 1]
            return carry

        lax.fori_loop(0, NB, coefficients, 0)
        c = jnp.zeros(line, F32)
        for b in range(NB):
            a00, a70, a07, a77 = kh[b], ks[b], kia[b], kc[b]
            inv = recip(1.0 - a00 * c)
            mixed = a70 * c * inv
            rb = row_of(r_before, b * ZL)
            ra = row_of(r_after, b * ZL + ZL - 1)
            p00 = 1.0 + a00 * rb
            p07 = a07 * ra
            ku0[b] = a70 * rb + mixed * p00
            ku7[b] = 1.0 + a77 * ra + mixed * p07
            kv0[b] = inv * p00
            kv7[b] = inv * p07
            ks[b] = a70 * inv
            kh[b] = a00 * inv
            kia[b] = a07 * inv
            c = a77 + mixed * a07
            kc[b] = c

    small = (KB, LANES)
    lanes = lax.broadcasted_iota(jnp.int32, small, 1)
    lane8 = lax.broadcasted_iota(jnp.int32, (8, LANES), 1)
    at_z = [lax.div(lax.rem(lanes, 16), 2) == z for z in range(ZL)]
    zero = jnp.zeros(small, F32)
    near = {}

    def ends(c):
        wait_all(precv.at[c, 0 : NB - 1], precv_s.at[c])

        tile8 = jnp.zeros((8, LANES), F32)
        odd = lax.rem(lane8, 2) == 1

        def gathered(h, t):
            value = tile8
            for p in range(NB):
                first = YL * p - LANES * t
                if first + YL <= 0 or first >= LANES:
                    continue
                piece = rolled(precv[c, p], first - LANES // 2 * h)
                value = jnp.where((lane8 >= first) & (lane8 < first + YL), piece, value)
            return value

        def beside(h, t):
            value = tile8
            for p in range(8 * t, 8 * t + 8):
                at_p = lax.div(lane8, 16) == p - 8 * t
                first = 16 * (p - 8 * t) - LANES // 2 * h - YL
                if p > 0:
                    value = jnp.where(at_p & ~odd, rolled(precv[c, p - 1], first - 1), value)
                if p < NB - 1:
                    value = jnp.where(at_p & odd, rolled(precv[c, p + 1], first + 1), value)
            return value

        planes = jnp.concatenate(
            [jnp.concatenate([gathered(h, t) for t in range(CH)], axis=1) for h in range(2)], axis=0
        )
        near[c] = [jnp.concatenate([beside(h, t) for h in range(2)], axis=0) for t in range(2)]
        rows = jnp.concatenate(
            [jnp.concatenate([jnp.where(at_z[z], v, 0.0) for v in near[c]], axis=1) for z in range(ZL)], axis=0
        )
        if c == 0:
            need("win", "sin")
        rhy[c] = by_table(rows, win[0], win[1]).reshape(ZL, KB, N)
        v = by_table(planes, sin_r[0], sin_r[1])
        first, last = solve(lambda z: rhy[c, z], eg.at[c], gwork.at[c])
        q = (first + jnp.where(core == 0, v, 0.0), last + jnp.where(core == 0, 0.0, v))
        for s in range(NS):
            rt, lt = divmod(s, CH)
            for i in range(2):
                qbuf[c, s, i] = q[i][8 * rt : 8 * rt + 8, lt * LANES : (lt + 1) * LANES]
        for d in GZ_ORDER:
            g = peer(gz, d)

            @pl.when(solves(g))
            def _():
                remote(qbuf.at[c, place(g)], qrecv.at[c, gz], qsend_s.at[c], qrecv_s.at[c], {"gz": g}).start()

        @pl.when(is_solver)
        def _():
            qrecv[c, gz] = qbuf[c, me_s]

    def chain(c):
        wait_all(qrecv.at[c, 0 : NB - 1], qrecv_s.at[c])
        part = slice(8 * c, 8 * c + 8)

        def row8(ref, i):
            return jnp.broadcast_to(ref[i : i + 1, :], (8, LANES))

        s = None
        for b in range(NB):
            q0, q7 = qrecv[c, b, 0], qrecv[c, b, 1]
            h = kv0[b, part] * q0 + kv7[b, part] * q7
            v = ku0[b, part] * q0 + ku7[b, part] * q7
            if b:
                h = h + kh[b, part] * s
                v = v + ks[b, part] * s
            s = v
            hh[b] = h
            ss[b] = s
        upper = None
        for b in range(NB - 1, -1, -1):
            head = hh[b]
            tail = ss[b]
            if b < NB - 1:
                head = head + kia[b, part] * upper
                tail = tail + kc[b, part] * upper
            hh[b] = head
            ss[b] = tail
            upper = head
        for b in range(NB):
            low = row8(r_before, b * ZL) * hh[b]
            if b:
                low = low + ss[b - 1]
            high = row8(r_after, b * ZL + ZL - 1) * ss[b]
            if b < NB - 1:
                high = high + hh[b + 1]
            rbuf[c, b, 0] = row8(alpha, b * ZL) * low
            rbuf[c, b, 1] = row8(beta, b * ZL + ZL - 1) * high
        for d in GZ_ORDER:
            g = peer(gz, d)
            remote(rbuf.at[c, g], rrecv.at[c, me_s], rsend_s.at[c], rrecv_s.at[c], {"gz": g}).start()
        rrecv[c, me_s] = rbuf[c, gz]

    def inner(c):
        @pl.when(is_solver)
        def _():
            wait_all(rrecv.at[c, 0 : NS - 1], rrecv_s.at[c])

        @pl.when(jnp.logical_not(is_solver))
        def _():
            wait_all(rrecv.at[c], rrecv_s.at[c])

        low, high = (
            jnp.concatenate(
                [jnp.concatenate([rrecv[c, CH * rt + lt, i] for lt in range(CH)], axis=1) for rt in range(2)], axis=0
            )
            for i in range(2)
        )
        ends_of = {0: low, ZL - 1: high}
        solve(lambda z: rhy[c, z] + ends_of[z] if z in ends_of else rhy[c, z], eg.at[c], gwork.at[c])
        if c == 0:
            need("wout")
        r = by_table((gwork[c].reshape(ZL * KB, N)), wout[0], wout[1])
        planes = by_table(jnp.where(core == 0, low, high), sin_r[0], sin_r[1])
        edge = []
        for t in range(2):
            value = near[c][t]
            for z in range(ZL):
                value = value + jnp.where(at_z[z], r[z * KB : (z + 1) * KB, t * LANES : (t + 1) * LANES], 0.0)
            edge.append(value)
        for p in range(NB):
            value = jnp.zeros((8, LANES), F32)
            for h in range(2):
                part = slice(8 * h, 8 * h + 8)
                base = h * LANES // 2
                for t in range(YL * p // LANES, (YL * p + YL - 1) // LANES + 1):
                    move = base - YL * p
                    first = max(LANES * t, YL * p) + move
                    stop = min(LANES * (t + 1), YL * p + YL) + move
                    piece = rolled(planes[part, t * LANES : (t + 1) * LANES], LANES * t + move)
                    value = jnp.where((lane8 >= first) & (lane8 < stop), piece, value)
                first = base + YL
                piece = rolled(edge[p // 8][part], first - 16 * (p % 8))
                value = jnp.where((lane8 >= first) & (lane8 < first + 16), piece, value)
            bbuf[c, p] = value
        for d in PA_ORDER:
            p = peer(pa, d)
            remote(bbuf.at[c, p], brecv.at[c, rows_of(pa), :], bsend_s.at[c], brecv_s.at[c], {"pa": p}).start()
        brecv[c, rows_of(pa), :] = bbuf[c, pa]

    def again(c):
        wait_all(bbuf.at[c, 0 : NB - 1], brecv_s.at[c])
        if c == 0:
            need("mc", "bwd")
        half = LANES // 2
        x = jnp.transpose(brecv[c])
        a, b = cut(jnp.concatenate([x[:half], x[half:]], axis=1))
        add = dot(mc[...], jnp.concatenate([a, b, a], axis=0))
        for z in range(ZL):
            fh[c, z] = fh[c, z] + add[z * YL : (z + 1) * YL]
        alone(c, 1)
        exchange(c, 1)

    def finish(*batches):
        us = []
        for c in batches:
            paired(c, 1)
            us.append(jnp.concatenate([sines(work[c, z]) for z in range(ZL)], axis=0))
        u = jnp.concatenate(us, axis=1)
        rows = slice(batches[0] * CW, (batches[-1] + 1) * CW)
        part = stacked(*cut(u), bwd[0, rows], bwd[1, rows])
        if batches[0] == 0:
            out[...] = part
        else:
            out[...] += part

    for c in range(NC):
        ends(c)
    for c in range(NC):
        pl.when(is_solver)(functools.partial(chain, c))
    for c in range(NC):
        inner(c)
    again(0)
    finish(0)
    again(1)
    again(2)
    finish(1)
    finish(2)

    wait_all(widths.at[0 : NB - 1], send_s.at[0])
    wait_all(wother, send_s.at[1])
    for c in range(NC):
        wait_all(precv.at[c, 0 : NB - 1], psend_s.at[c])
        wait_all(bbuf.at[c, 0 : NB - 1], bsend_s.at[c])
        for i in range(2):
            wait_all(xbuf.at[i, c], xsend_s.at[i, c])

        @pl.when(jnp.logical_not(is_solver))
        def _():
            wait_all(qbuf.at[c], qsend_s.at[c])

        @pl.when(is_solver)
        def _():
            wait_all(qbuf.at[c, 0 : NS - 1], qsend_s.at[c])
            wait_all(rbuf.at[c, 0 : NB - 1], rsend_s.at[c])


def on_device(source, cell_width):
    t = tables()
    args = [jnp.asarray(t[name]) for name in TABLES]
    hbm = pl.BlockSpec(memory_space=pltpu.HBM)
    v = pltpu.VMEM
    dma = pltpu.SemaphoreType.DMA
    here = [v(x.shape[1:] if n in ("mc", "mct") else x.shape, x.dtype) for n, x in zip(TABLES[:-1], args)] + [v((NC, 2, 8, LANES), F32)]
    coef = v((NB, 8 * NC, LANES), F32)
    out = pl.pallas_call(
        kernel,
        out_shape=jax.ShapeDtypeStruct((ZL * YL, N), F32),
        in_specs=[hbm, pl.BlockSpec(memory_space=pltpu.SMEM)] + [hbm] * len(args),
        out_specs=pl.BlockSpec(memory_space=pltpu.VMEM),
        scratch_shapes=[v((ZL * YL, N), F32)]
        + here
        + [
            v((2 * ZL * YL, N), BF16),
            v((NC, ZL, YL, CW), F32),
            v((NC, ZL, YL, CW), F32),
            v((NC, ZL, YL, CW), F32),
            v((NC, LANES, LANES), F32),
            v((NC, NB, 8, LANES), F32),
            v((ZL, LANES), F32),
            v((ZL, LANES), F32),
            v((NB, ZL, LANES), F32),
        ]
        + [v((NB * ZL, LANES), F32)] * 4
        + [
            v((NC, ZL, KB, N), F32),
            v((NC, ZL, KB, N), F32),
            v((NC, ZL, KB, N), F32),
            v((NC, NS, 2, 8, LANES), F32),
            v((NC, NB, 2, 8, LANES), F32),
            v((NC, NB, 2, 8, LANES), F32),
            v((NC, NS, 2, 8, LANES), F32),
        ]
        + [coef] * 8
        + [
            v((NB, 8, LANES), F32),
            v((NB, 8, LANES), F32),
            v((NC, NB, 8, LANES), F32),
            v((NC, LANES, LANES), F32),
        ]
        + [v((NC, YL, CW), F32)] * 2
        + [v((2, NC, YL, CW), F32)] * 2
        + [
            dma((24,)),
            dma((2,)),
            dma((2,)),
        ]
        + [dma((NC,))] * 8
        + [dma((2, NC))] * 2,
        compiler_params=pltpu.CompilerParams(
            collective_id=0, has_side_effects=True, vmem_limit_bytes=44 * 1024 * 1024
        ),
        name="poisson",
    )(*(pltpu.with_memory_space_constraint(x, pltpu.HBM) for x in (source.reshape(ZL * YL, N), cell_width, *args)))
    return out.reshape(ZL, YL, N)


def solution(mesh):
    return jax.shard_map(
        on_device,
        mesh=mesh,
        in_specs=(P("gz", "pa", None), P("gz")),
        out_specs=P("gz", "pa", None),
        check_vma=False,
    )
```

```python
import functools

import jax
import jax.numpy as jnp
import numpy as np
from jax import lax
from jax.experimental import pallas as pl
from jax.experimental.pallas import tpu as pltpu
from jax.sharding import PartitionSpec as P

F32 = jnp.float32
BF16 = jnp.bfloat16
N = 768
NB = 16
ZL = 8
YL = 48
LANES = 128
CH = N // LANES
NC = 3
CW = N // NC
KB = CW // NB
IDLE = (0, 4, 10, 14)
PA_ORDER = (4, 12, 3, 5, 11, 13, 2, 6, 10, 14, 1, 7, 9, 15, 8)
GZ_ORDER = (12, 4, 11, 13, 5, 3, 10, 14, 6, 2, 7, 9, 8, 15, 1)
SOLVERS = tuple(g for g in range(NB) if g not in IDLE)
NS = len(SOLVERS)


def split64(x):
    hi = x.astype(np.float32).astype(jnp.bfloat16)
    lo = (x - hi.astype(np.float64)).astype(np.float32).astype(jnp.bfloat16)
    return np.stack([hi, lo])


@functools.cache
def tables():
    n = np.arange(N)
    phases = n[:, None] * (2 * n[None, :] + 1) % (4 * N)
    weights = np.where(n == 0, np.sqrt(1.0 / N), np.sqrt(2.0 / N))
    cos_t = weights[:, None] * np.cos(phases * (np.pi / (2 * N)))

    def sine(width, rows, cols):
        p = rows[:, None] * cols[None, :] % (2 * (width + 1))
        return np.sqrt(2.0 / (width + 1)) * np.sin(p * (np.pi / (width + 1)))

    m = n + 1
    sin_t = sine(N, m, m)
    ml = np.arange(1, YL + 1)
    s48 = sine(YL, ml, ml)
    hi, lo = split64(s48)
    s48st = np.concatenate([hi, hi, lo], axis=1)
    mcp = np.zeros((2, ZL * YL, LANES // 2))
    mcp[0, :YL, :YL] = s48
    mcp[1, (ZL - 1) * YL :, :YL] = s48
    for z in range(ZL):
        mcp[:, z * YL : (z + 1) * YL, YL + 2 * z] = s48[:, 0]
        mcp[:, z * YL : (z + 1) * YL, YL + 2 * z + 1] = s48[:, YL - 1]
    own = np.zeros((NB, ZL, 2, N))
    beside = np.zeros((NB, ZL, 2, N))
    for p in range(NB):
        for e in range(2):
            row = YL * p + (YL - 1) * e
            own[p, :, e] = sin_t[row]
            near = row + (1 if e else -1)
            if 0 <= near < N:
                beside[p, :, e] = sin_t[near]
    own = own.reshape(2 * ZL * NB, N)
    beside = beside.reshape(2 * ZL * NB, N)
    lam_k = 4 * np.sin(n * np.pi / (2 * N)) ** 2
    lam_l = 4 * np.sin(m * np.pi / (2 * (N + 1))) ** 2
    lam_s = 4 * np.sin(ml * np.pi / (2 * (YL + 1))) ** 2
    rows = np.zeros((8, N), np.float32)
    rows[0] = lam_k
    rows[1] = lam_l
    cos2 = split64(cos_t)
    return dict(
        fwd=np.ascontiguousarray(cos2.reshape(2, NC, CW, N).transpose(1, 0, 3, 2)),
        bwd=cos2,
        sin=split64(sin_t),
        s48=s48st,
        mct=split64(mcp.transpose(0, 2, 1).copy()).transpose(1, 0, 2, 3).reshape(2, LANES, ZL * YL),
        mc=np.concatenate([split64(mcp)[i] for i in (0, 0, 1)], axis=2),
        win=split64(own),
        wout=split64(beside.T.copy()),
        rows=rows,
        lam_s=np.broadcast_to(lam_s[:, None], (YL, CW)).astype(np.float32),
        lam_k=np.broadcast_to(lam_k[:, None], (N, LANES)).astype(np.float32).reshape(NC * 2 * NB, 8, LANES),
    )


TABLES = ("fwd", "bwd", "sin", "s48", "mct", "mc", "win", "wout", "rows", "lam_s", "lam_k")


def cut(x):
    hi = x.astype(BF16)
    return hi, (x - hi.astype(F32)).astype(BF16)


def dot(a, b):
    return jnp.dot(a, b, preferred_element_type=F32)


def by_table(x, hi, lo):
    a, b = cut(x)
    m = x.shape[0]
    r = dot(jnp.concatenate([a, b], axis=0), hi)
    return r[:m] + r[m:] + dot(a, lo)


def table_by(t, x):
    a, b = cut(x)
    m = t.shape[0] // 2
    r = dot(t, a)
    return r[:m] + r[m:] + dot(t[:m], b)


def recip(x):
    return 1.0 / x


def remote(src, dst, send, recv, where):
    return pltpu.make_async_remote_copy(
        src_ref=src,
        dst_ref=dst,
        send_sem=send,
        recv_sem=recv,
        device_id=where,
        device_id_type=pl.DeviceIdType.MESH,
    )


def rolled(x, shift):
    shift %= LANES
    return x if shift == 0 else pltpu.roll(x, shift, axis=1)


def wide(row, like):
    return jnp.broadcast_to(jnp.concatenate([row] * (like[1] // LANES), axis=1), like)


def kernel(
    src_h, cw, fwd_h, bwd_h, sin_h, s48_h, mct_h, mc_h, win_h, wout_h, rows_h, lam_s_h, lam_k_h, out,
    src, fwd, bwd, sin_r, s48, mct, mc, win, wout, lam_rows, lam_s, lam_k,
    s_st, fh, work, eloc, pbuf, precv, wmine, wother, widths, alpha, beta, r_before, r_after,
    rhy, eg, gwork, qbuf, qrecv, rbuf, rrecv, ks, ku0, ku7, kv0, kv7, kh, kia, kc, hh, ss, bbuf, brecv,
    m_own, m_other, xbuf, xrecv,
    load_s, send_s, recv_s, psend_s, precv_s, qsend_s, qrecv_s, rsend_s, rrecv_s, bsend_s, brecv_s, xsend_s, xrecv_s,
):
    pa = lax.axis_index("pa")
    gz = lax.axis_index("gz")
    core = lax.rem(gz, 2)

    def peer(me, d):
        return lax.rem(me + d, NB)

    loads = {}

    def load(name, h, v):
        loads[name] = pltpu.make_async_copy(h, v, load_s.at[len(loads)])
        loads[name].start()

    def need(*names):
        for name in names:
            loads[name].wait()

    load("rows", rows_h, lam_rows)
    load("lam_s", lam_s_h, lam_s)
    load("src", src_h, src)
    load("fwd0", fwd_h.at[0], fwd.at[0])
    load("s48", s48_h, s48)
    load("mct", mct_h.at[core], mct)
    for c in range(NC):
        for h in range(2):
            load("lam_k%d" % (2 * c + h), lam_k_h.at[NB * (2 * c + h) + pa], lam_k.at[c, h])

    barrier = pltpu.get_barrier_semaphore()
    for d in range(1, NB):
        pl.semaphore_signal(barrier, inc=1, device_id={"pa": peer(pa, d)}, device_id_type=pl.DeviceIdType.MESH)
        pl.semaphore_signal(barrier, inc=1, device_id={"gz": peer(gz, d)}, device_id_type=pl.DeviceIdType.MESH)

    for z in range(ZL):
        wmine[z : z + 1, :] = jnp.full((1, LANES), cw[z], F32)
    def own_links(w):
        at = lax.broadcasted_iota(jnp.int32, (ZL, LANES), 0)
        al = 2.0 / ((jnp.where(at == 0, w, pltpu.roll(w, 1, axis=0)) + w) * w)
        be = 2.0 / ((w + jnp.where(at == ZL - 1, w, pltpu.roll(w, ZL - 1, axis=0))) * w)
        return al, be

    al_b, be_b = own_links(wmine[...])

    def a_of(z, like):
        return wide(al_b[z : z + 1, :], like)

    def b_of(z, like):
        return wide(be_b[z : z + 1, :], like)

    def factor(e_ref, lam):
        like = lam.shape
        e = None
        for z in range(ZL):
            d = a_of(z, like) + b_of(z, like) + lam
            if z:
                d = d - a_of(z, like) * b_of(z - 1, like) * e
            e = recip(d)
            e_ref[z] = e

    def solve(rhs_of, e_ref, x_ref):
        like = x_ref.shape[1:]
        y = None
        for z in range(ZL):
            r = rhs_of(z)
            if z:
                r = r + a_of(z, like) * y
            y = e_ref[z] * r
            x_ref[z] = y
        last = y
        for z in range(ZL - 2, -1, -1):
            y = x_ref[z] + e_ref[z] * b_of(z, like) * y
            x_ref[z] = y
        return y, last

    need("rows", "lam_s")
    for c in range(NC):
        factor(eloc.at[c], lam_s[...] + lam_rows[0:1, c * CW : (c + 1) * CW])
    need("src", "s48")
    load("fwd1", fwd_h.at[1], fwd.at[1])
    load("fwd2", fwd_h.at[2], fwd.at[2])
    s_st[0 : ZL * YL], s_st[ZL * YL :] = cut(src[...])

    def sines(x):
        a, b = cut(x)
        return dot(s48[...], jnp.concatenate([a, b, a], axis=0))

    def rows_of(q):
        return pl.ds(pl.multiple_of(q * 8, 8), 8)

    def wait_all(ref, sem):
        pltpu.make_async_copy(ref, ref, sem).wait()

    partner = {"gz": gz + 1 - 2 * core}

    def pair(c):
        w_o = wother[...]
        w_m = wmine[...]
        al_o, be_o = own_links(w_o)
        like = (YL, CW)

        def by_core(x, y):
            return jnp.where(core == 0, x, y)

        w_l, w_u = by_core(w_m, w_o), by_core(w_o, w_m)
        al_l, be_l = by_core(al_b, al_o), by_core(be_b, be_o)
        al_u, be_u = by_core(al_o, al_b), by_core(be_o, be_b)

        def row(x, z):
            return wide(x[z : z + 1, :], like)

        link_l = 2.0 / ((w_l[ZL - 1 : ZL] + w_u[0:1]) * w_l[ZL - 1 : ZL])
        link_u = 2.0 / ((w_l[ZL - 1 : ZL] + w_u[0:1]) * w_u[0:1])
        more_l = wide(be_l[ZL - 1 : ZL] - link_l, like)
        more_u = wide(al_u[0:1] - link_u, like)
        link_l = wide(link_l, like)
        link_u = wide(link_u, like)
        lam = lam_s[...] + lam_rows[0:1, c * CW : (c + 1) * CW]
        g_l = recip(row(al_l, 0) + row(be_l, 0) + lam)
        for z in range(1, ZL):
            g_l = recip(row(al_l, z) + row(be_l, z) + lam - row(al_l, z) * row(be_l, z - 1) * g_l)
        g_u = recip(row(al_u, ZL - 1) + row(be_u, ZL - 1) + lam)
        for z in range(ZL - 2, -1, -1):
            g_u = recip(row(al_u, z) + row(be_u, z) + lam - row(be_u, z) * row(al_u, z + 1) * g_u)
        rest_l = 1.0 - g_l * more_l
        rest_u = 1.0 - g_u * more_u
        inv = recip(rest_l * rest_u - g_l * g_u * link_l * link_u)
        own_l = link_l * link_u * g_u + more_l * rest_u
        own_u = link_l * link_u * g_l + more_u * rest_l
        m_own[c] = by_core(own_l, own_u) * inv
        m_other[c] = by_core(link_l, link_u) * inv

    def alone(c, i):
        first, last = solve(lambda z: fh[c, z], eloc.at[c], work.at[c])
        xbuf[i, c] = jnp.where(core == 0, last, first)

    def exchange(c, i):
        remote(xbuf.at[i, c], xrecv.at[i, c], xsend_s.at[i, c], xrecv_s.at[i, c], partner).start()

    def paired(c, i):
        wait_all(xrecv.at[i, c], xrecv_s.at[i, c])
        more = m_own[c] * xbuf[i, c] + m_other[c] * xrecv[i, c]
        ends_of = {0: jnp.where(core == 0, 0.0, more), ZL - 1: jnp.where(core == 0, more, 0.0)}
        solve(lambda z: fh[c, z] + ends_of[z] if z in ends_of else fh[c, z], eloc.at[c], work.at[c])

    def block(c):
        need("fwd%d" % c)
        f = dot(s_st[...], fwd[c, 0])
        f = f[: ZL * YL] + f[ZL * YL :] + dot(s_st[0 : ZL * YL], fwd[c, 1])
        for z in range(ZL):
            fh[c, z] = sines(f[z * YL : (z + 1) * YL])
        alone(c, 0)

    def perimeter(c):
        paired(c, 0)
        if c == 0:
            need("mct")
        p = table_by(mct[...], work[c].reshape(ZL * YL, CW))
        pbuf[c] = jnp.transpose(jnp.concatenate([p[:, :LANES], p[:, LANES:]], axis=0))
        for d in PA_ORDER:
            q = peer(pa, d)
            remote(pbuf.at[c, rows_of(q), :], precv.at[c, pa], psend_s.at[c], precv_s.at[c], {"pa": q}).start()
        precv[c, pa] = pbuf[c, rows_of(pa), :]

    block(0)
    load("win", win_h, win)
    load("sin", sin_h, sin_r)
    load("wout", wout_h, wout)
    load("mc", mc_h.at[core], mc)
    load("bwd", bwd_h, bwd)
    pl.semaphore_wait(barrier, 2 * (NB - 1))
    remote(wmine, wother, send_s.at[1], recv_s.at[1], partner).start()
    exchange(0, 0)
    for d in GZ_ORDER:
        remote(wmine, widths.at[gz], send_s.at[0], recv_s.at[0], {"gz": peer(gz, d)}).start()
    widths[gz] = wmine[...]
    block(1)
    exchange(1, 0)
    wait_all(wother, recv_s.at[1])
    pair(0)
    perimeter(0)
    block(2)
    exchange(2, 0)
    pair(1)
    perimeter(1)
    pair(2)
    perimeter(2)

    need(*("lam_k%d" % c for c in range(2 * NC)))
    for c in range(NC):
        factor(eg.at[c], wide(lam_k[c].reshape(KB, LANES), (KB, N)) + lam_rows[1:2, :])

    wait_all(widths.at[0 : NB - 1], recv_s.at[0])
    w = widths[...].reshape(NB * ZL, LANES)
    at = lax.broadcasted_iota(jnp.int32, (NB * ZL, LANES), 0)
    before = jnp.where(at == 0, 0.0, pltpu.roll(w, 1, axis=0))
    after = jnp.where(at == NB * ZL - 1, 0.0, pltpu.roll(w, NB * ZL - 1, axis=0))
    alpha[...] = 2.0 / ((before + w) * w)
    beta[...] = 2.0 / ((w + after) * w)
    r_before[...] = (before - w) / (2.0 * w)
    r_after[...] = (after - w) / (2.0 * w)

    def place(g):
        return g - sum(((g > i).astype(jnp.int32) for i in IDLE), jnp.int32(0))

    def solves(g):
        return functools.reduce(lambda x, y: x & y, [g != i for i in IDLE])

    me_s = place(gz)
    is_solver = solves(gz)
    line = (8 * NC, LANES)

    def row_of(ref, i):
        return jnp.broadcast_to(ref[pl.ds(i, 1), :], line)

    @pl.when(is_solver)
    def _():
        rt = lax.div(me_s, CH)
        lt = lax.rem(me_s, CH)
        lam = jnp.concatenate([lam_k[c, rt] for c in range(NC)], axis=0)
        lam = lam + lam_rows[1:2, pl.ds(pl.multiple_of(lt * LANES, LANES), LANES)]

        def coefficients(b, carry):
            al = [row_of(alpha, b * ZL + z) for z in range(ZL)]
            be = [row_of(beta, b * ZL + z) for z in range(ZL)]
            e = recip(al[0] + be[0] + lam)
            prod_e = e
            prod_b = be[0]
            for z in range(1, ZL):
                e = recip(al[z] + be[z] + lam - al[z] * be[z - 1] * e)
                prod_e = prod_e * e * al[z]
                prod_b = prod_b * be[z] / al[z]
            g = recip(al[ZL - 1] + be[ZL - 1] + lam)
            for z in range(ZL - 2, -1, -1):
                g = recip(al[z] + be[z] + lam - be[z] * al[z + 1] * g)
            kh[b] = g * al[0]
            ks[b] = prod_e * al[0]
            kia[b] = prod_e * prod_b
            kc[b] = e * be[ZL - 1]
            return carry

        lax.fori_loop(0, NB, coefficients, 0)
        c = jnp.zeros(line, F32)
        for b in range(NB):
            a00, a70, a07, a77 = kh[b], ks[b], kia[b], kc[b]
            inv = recip(1.0 - a00 * c)
            mixed = a70 * c * inv
            rb = row_of(r_before, b * ZL)
            ra = row_of(r_after, b * ZL + ZL - 1)
            p00 = 1.0 + a00 * rb
            p07 = a07 * ra
            ku0[b] = a70 * rb + mixed * p00
            ku7[b] = 1.0 + a77 * ra + mixed * p07
            kv0[b] = inv * p00
            kv7[b] = inv * p07
            ks[b] = a70 * inv
            kh[b] = a00 * inv
            kia[b] = a07 * inv
            c = a77 + mixed * a07
            kc[b] = c

    small = (KB, LANES)
    lanes = lax.broadcasted_iota(jnp.int32, small, 1)
    lane8 = lax.broadcasted_iota(jnp.int32, (8, LANES), 1)
    at_z = [lax.div(lax.rem(lanes, 16), 2) == z for z in range(ZL)]
    zero = jnp.zeros(small, F32)
    near = {}

    def ends(c):
        wait_all(precv.at[c, 0 : NB - 1], precv_s.at[c])

        tile8 = jnp.zeros((8, LANES), F32)
        odd = lax.rem(lane8, 2) == 1

        def gathered(h, t):
            value = tile8
            for p in range(NB):
                first = YL * p - LANES * t
                if first + YL <= 0 or first >= LANES:
                    continue
                piece = rolled(precv[c, p], first - LANES // 2 * h)
                value = jnp.where((lane8 >= first) & (lane8 < first + YL), piece, value)
            return value

        def beside(h, t):
            value = tile8
            for p in range(8 * t, 8 * t + 8):
                at_p = lax.div(lane8, 16) == p - 8 * t
                first = 16 * (p - 8 * t) - LANES // 2 * h - YL
                if p > 0:
                    value = jnp.where(at_p & ~odd, rolled(precv[c, p - 1], first - 1), value)
                if p < NB - 1:
                    value = jnp.where(at_p & odd, rolled(precv[c, p + 1], first + 1), value)
            return value

        planes = jnp.concatenate(
            [jnp.concatenate([gathered(h, t) for t in range(CH)], axis=1) for h in range(2)], axis=0
        )
        near[c] = [jnp.concatenate([beside(h, t) for h in range(2)], axis=0) for t in range(2)]
        rows = jnp.concatenate(
            [jnp.concatenate([jnp.where(at_z[z], v, 0.0) for v in near[c]], axis=1) for z in range(ZL)], axis=0
        )
        if c == 0:
            need("win", "sin")
        rhy[c] = by_table(rows, win[0], win[1]).reshape(ZL, KB, N)
        v = by_table(planes, sin_r[0], sin_r[1])
        first, last = solve(lambda z: rhy[c, z], eg.at[c], gwork.at[c])
        q = (first + jnp.where(core == 0, v, 0.0), last + jnp.where(core == 0, 0.0, v))
        for s in range(NS):
            rt, lt = divmod(s, CH)
            for i in range(2):
                qbuf[c, s, i] = q[i][8 * rt : 8 * rt + 8, lt * LANES : (lt + 1) * LANES]
        for d in GZ_ORDER:
            g = peer(gz, d)

            @pl.when(solves(g))
            def _():
                remote(qbuf.at[c, place(g)], qrecv.at[c, gz], qsend_s.at[c], qrecv_s.at[c], {"gz": g}).start()

        @pl.when(is_solver)
        def _():
            qrecv[c, gz] = qbuf[c, me_s]

    def chain(c):
        wait_all(qrecv.at[c, 0 : NB - 1], qrecv_s.at[c])
        part = slice(8 * c, 8 * c + 8)

        def row8(ref, i):
            return jnp.broadcast_to(ref[i : i + 1, :], (8, LANES))

        s = None
        for b in range(NB):
            q0, q7 = qrecv[c, b, 0], qrecv[c, b, 1]
            h = kv0[b, part] * q0 + kv7[b, part] * q7
            v = ku0[b, part] * q0 + ku7[b, part] * q7
            if b:
                h = h + kh[b, part] * s
                v = v + ks[b, part] * s
            s = v
            hh[b] = h
            ss[b] = s
        upper = None
        for b in range(NB - 1, -1, -1):
            head = hh[b]
            tail = ss[b]
            if b < NB - 1:
                head = head + kia[b, part] * upper
                tail = tail + kc[b, part] * upper
            hh[b] = head
            ss[b] = tail
            upper = head
        for b in range(NB):
            low = row8(r_before, b * ZL) * hh[b]
            if b:
                low = low + ss[b - 1]
            high = row8(r_after, b * ZL + ZL - 1) * ss[b]
            if b < NB - 1:
                high = high + hh[b + 1]
            rbuf[c, b, 0] = row8(alpha, b * ZL) * low
            rbuf[c, b, 1] = row8(beta, b * ZL + ZL - 1) * high
        for d in GZ_ORDER:
            g = peer(gz, d)
            remote(rbuf.at[c, g], rrecv.at[c, me_s], rsend_s.at[c], rrecv_s.at[c], {"gz": g}).start()
        rrecv[c, me_s] = rbuf[c, gz]

    def inner(c):
        @pl.when(is_solver)
        def _():
            wait_all(rrecv.at[c, 0 : NS - 1], rrecv_s.at[c])

        @pl.when(jnp.logical_not(is_solver))
        def _():
            wait_all(rrecv.at[c], rrecv_s.at[c])

        low, high = (
            jnp.concatenate(
                [jnp.concatenate([rrecv[c, CH * rt + lt, i] for lt in range(CH)], axis=1) for rt in range(2)], axis=0
            )
            for i in range(2)
        )
        ends_of = {0: low, ZL - 1: high}
        solve(lambda z: rhy[c, z] + ends_of[z] if z in ends_of else rhy[c, z], eg.at[c], gwork.at[c])
        if c == 0:
            need("wout")
        r = by_table((gwork[c].reshape(ZL * KB, N)), wout[0], wout[1])
        planes = by_table(jnp.where(core == 0, low, high), sin_r[0], sin_r[1])
        edge = []
        for t in range(2):
            value = near[c][t]
            for z in range(ZL):
                value = value + jnp.where(at_z[z], r[z * KB : (z + 1) * KB, t * LANES : (t + 1) * LANES], 0.0)
            edge.append(value)
        for p in range(NB):
            value = jnp.zeros((8, LANES), F32)
            for h in range(2):
                part = slice(8 * h, 8 * h + 8)
                base = h * LANES // 2
                for t in range(YL * p // LANES, (YL * p + YL - 1) // LANES + 1):
                    move = base - YL * p
                    first = max(LANES * t, YL * p) + move
                    stop = min(LANES * (t + 1), YL * p + YL) + move
                    piece = rolled(planes[part, t * LANES : (t + 1) * LANES], LANES * t + move)
                    value = jnp.where((lane8 >= first) & (lane8 < stop), piece, value)
                first = base + YL
                piece = rolled(edge[p // 8][part], first - 16 * (p % 8))
                value = jnp.where((lane8 >= first) & (lane8 < first + 16), piece, value)
            bbuf[c, p] = value
        for d in PA_ORDER:
            p = peer(pa, d)
            remote(bbuf.at[c, p], brecv.at[c, rows_of(pa), :], bsend_s.at[c], brecv_s.at[c], {"pa": p}).start()
        brecv[c, rows_of(pa), :] = bbuf[c, pa]

    def again(c):
        wait_all(bbuf.at[c, 0 : NB - 1], brecv_s.at[c])
        if c == 0:
            need("mc", "bwd")
        half = LANES // 2
        x = jnp.transpose(brecv[c])
        a, b = cut(jnp.concatenate([x[:half], x[half:]], axis=1))
        add = dot(mc[...], jnp.concatenate([a, b, a], axis=0))
        for z in range(ZL):
            fh[c, z] = fh[c, z] + add[z * YL : (z + 1) * YL]
        alone(c, 1)
        exchange(c, 1)

    def finish(*batches):
        us = []
        for c in batches:
            paired(c, 1)
            us.append(jnp.concatenate([sines(work[c, z]) for z in range(ZL)], axis=0))
        u = jnp.concatenate(us, axis=1)
        rows = slice(batches[0] * CW, (batches[-1] + 1) * CW)
        part = by_table(u, bwd[0, rows], bwd[1, rows])
        if batches[0] == 0:
            out[...] = part
        else:
            out[...] += part

    for c in range(NC):
        ends(c)
    for c in range(NC):
        pl.when(is_solver)(functools.partial(chain, c))
    for c in range(NC):
        inner(c)
    again(0)
    finish(0)
    again(1)
    again(2)
    finish(1)
    finish(2)

    wait_all(widths.at[0 : NB - 1], send_s.at[0])
    wait_all(wother, send_s.at[1])
    for c in range(NC):
        wait_all(precv.at[c, 0 : NB - 1], psend_s.at[c])
        wait_all(bbuf.at[c, 0 : NB - 1], bsend_s.at[c])
        for i in range(2):
            wait_all(xbuf.at[i, c], xsend_s.at[i, c])

        @pl.when(jnp.logical_not(is_solver))
        def _():
            wait_all(qbuf.at[c], qsend_s.at[c])

        @pl.when(is_solver)
        def _():
            wait_all(qbuf.at[c, 0 : NS - 1], qsend_s.at[c])
            wait_all(rbuf.at[c, 0 : NB - 1], rsend_s.at[c])


def on_device(source, cell_width):
    t = tables()
    args = [jnp.asarray(t[name]) for name in TABLES]
    hbm = pl.BlockSpec(memory_space=pltpu.HBM)
    v = pltpu.VMEM
    dma = pltpu.SemaphoreType.DMA
    here = [v(x.shape[1:] if n in ("mc", "mct") else x.shape, x.dtype) for n, x in zip(TABLES[:-1], args)] + [v((NC, 2, 8, LANES), F32)]
    coef = v((NB, 8 * NC, LANES), F32)
    out = pl.pallas_call(
        kernel,
        out_shape=jax.ShapeDtypeStruct((ZL * YL, N), F32),
        in_specs=[hbm, pl.BlockSpec(memory_space=pltpu.SMEM)] + [hbm] * len(args),
        out_specs=pl.BlockSpec(memory_space=pltpu.VMEM),
        scratch_shapes=[v((ZL * YL, N), F32)]
        + here
        + [
            v((2 * ZL * YL, N), BF16),
            v((NC, ZL, YL, CW), F32),
            v((NC, ZL, YL, CW), F32),
            v((NC, ZL, YL, CW), F32),
            v((NC, LANES, LANES), F32),
            v((NC, NB, 8, LANES), F32),
            v((ZL, LANES), F32),
            v((ZL, LANES), F32),
            v((NB, ZL, LANES), F32),
        ]
        + [v((NB * ZL, LANES), F32)] * 4
        + [
            v((NC, ZL, KB, N), F32),
            v((NC, ZL, KB, N), F32),
            v((NC, ZL, KB, N), F32),
            v((NC, NS, 2, 8, LANES), F32),
            v((NC, NB, 2, 8, LANES), F32),
            v((NC, NB, 2, 8, LANES), F32),
            v((NC, NS, 2, 8, LANES), F32),
        ]
        + [coef] * 8
        + [
            v((NB, 8, LANES), F32),
            v((NB, 8, LANES), F32),
            v((NC, NB, 8, LANES), F32),
            v((NC, LANES, LANES), F32),
        ]
        + [v((NC, YL, CW), F32)] * 2
        + [v((2, NC, YL, CW), F32)] * 2
        + [
            dma((24,)),
            dma((2,)),
            dma((2,)),
        ]
        + [dma((NC,))] * 8
        + [dma((2, NC))] * 2,
        compiler_params=pltpu.CompilerParams(
            collective_id=0, has_side_effects=True, vmem_limit_bytes=44 * 1024 * 1024
        ),
        name="poisson",
    )(*(pltpu.with_memory_space_constraint(x, pltpu.HBM) for x in (source.reshape(ZL * YL, N), cell_width, *args)))
    return out.reshape(ZL, YL, N)


def solution(mesh):
    return jax.shard_map(
        on_device,
        mesh=mesh,
        in_specs=(P("gz", "pa", None), P("gz")),
        out_specs=P("gz", "pa", None),
        check_vma=False,
    )
```
